32 devices in a mesh: gx: 8 (over z, y), gy: 4 (over x, core).
Axes of the slice: x: 2, y: 2, z: 4, core: 2. Of those that a mesh axis runs over, the one named last changes fastest.
Arguments:
- start_state: float32 [5, 64, 64, 256], P(None, 'gx', 'gy'), may hold values from -1.5 to 5.5, as said below
- section_state: float32 [5, 64, 64, 256], P(None, 'gx', 'gy'), may hold values from -1.5 to 5.5, as said below
- previous_speed: float32 [], replicated, may hold values from 1.2 to 2.4
Outputs:
- new_state: float32 [5, 64, 64, 256], P(None, 'gx', 'gy')
- next_speed: float32 [], replicated
The draws below stay inside these ranges and needn't reach their ends.
Inputs may be any that keep to these rules, and one draw needn't show every extreme that they name: `start_state`: density (component 0) lies in 0.7 to 1.3 and the pressure 0.4 (E - |momentum|^2 / (2 density)) in 0.6 to 1.2 in every cell. `section_state`: density (component 0) lies in 0.7 to 1.3 and the pressure 0.4 (E - |momentum|^2 / (2 density)) in 0.6 to 1.2 in every cell.
All inputs are finite; a program needn't handle non-finite values.
Results may differ from the reference program's by a relative error of at most 0.00002.
Values sent between devices are 32-bit elements; how exact they have to be, the bound alone decides.
A program may use at most 64 MiB of HBM per device.

```python
import math
import jax
import jax.numpy as jnp

CX = 8
CY = 16
NZ = 256
NX = 64
NY = 64


GAMMA = 1.4


def periodic_offset(count, centre):
    offset = (jnp.arange(count, dtype=jnp.int32) - centre + count // 2) % count - count // 2
    return offset.astype(jnp.float32)


def bump_field(base_key):
    subkeys = jax.random.split(jax.random.fold_in(base_key, 5), 3)
    centre_x = jax.random.randint(subkeys[0], (), 0, NX, dtype=jnp.int32)
    centre_y = jax.random.randint(subkeys[1], (), 0, NY, dtype=jnp.int32)
    centre_z = jax.random.randint(subkeys[2], (), 0, NZ, dtype=jnp.int32)
    wide_x = float(max(NX // 32, 2))
    wide_y = float(max(NY // 32, 2))
    wide_z = float(max(NZ // 16, 2))
    along_x = (periodic_offset(NX, centre_x) / wide_x) ** 2
    along_y = (periodic_offset(NY, centre_y) / wide_y) ** 2
    along_z = (periodic_offset(NZ, centre_z) / wide_z) ** 2
    exponent = along_x[:, None, None] + along_y[None, :, None] + along_z[None, None, :]
    return jnp.exp(-0.5 * exponent)


def make_state(key, base_key):
    subkeys = jax.random.split(key, 3)
    amplitude = (0.2 + 0.25 * bump_field(base_key))[None]
    jitter = jnp.clip(jax.random.normal(subkeys[0], (3, NX, NY, NZ), jnp.float32), -2.5, 2.5)
    flow_speed_vector = amplitude * jitter
    density = 1.0 + 0.3 * jax.random.uniform(subkeys[1], (NX, NY, NZ), jnp.float32, -1.0, 1.0)
    thermodynamic_load = 0.9 + 0.3 * jax.random.uniform(subkeys[2], (NX, NY, NZ), jnp.float32, -1.0, 1.0)
    energy = thermodynamic_load / (GAMMA - 1.0) + 0.5 * density * jnp.sum(flow_speed_vector * flow_speed_vector, axis=0)
    return jnp.concatenate([density[None], density[None] * flow_speed_vector, energy[None]], axis=0)


def draw_start_state(key, part):
    return make_state(jax.random.fold_in(key, 11), key)


def draw_section_state(key, part):
    return make_state(jax.random.fold_in(key, 23), key)


def setup_inputs(seed: int = 0) -> dict:
    key_list = jax.random.split(jax.random.key(seed), 4)
    start_state = draw_start_state(jax.random.fold_in(key_list[3], 71), 0)
    section_state = draw_section_state(jax.random.fold_in(key_list[3], 71), 0)
    previous_speed = jnp.clip(jnp.exp(jax.random.uniform(key_list[2], (), jnp.float32, math.log(1.2), math.log(2.4))), 1.2, 2.4)
    return {"start_state": start_state, "section_state": section_state, "previous_speed": previous_speed}


GAMMA = 1.4
COURANT = 0.3
VISCOSITY = 0.05
CONDUCTION = 0.07
FIRST = (0.8, -0.2, 4.0 / 105.0, -1.0 / 280.0)
SECOND = (1.6, -0.2, 8.0 / 315.0, -1.0 / 560.0)
CENTRE = -205.0 / 72.0

def primitive(conserved_variables):
    density = conserved_variables[0]
    flow_speed_vector = (conserved_variables[1] / density, conserved_variables[2] / density, conserved_variables[3] / density)
    kinetic = 0.5 * (flow_speed_vector[0] * flow_speed_vector[0] + flow_speed_vector[1] * flow_speed_vector[1] + flow_speed_vector[2] * flow_speed_vector[2])
    thermodynamic_load = (GAMMA - 1.0) * (conserved_variables[4] - density * kinetic)
    return (density, flow_speed_vector, kinetic, thermodynamic_load)

def wave_speed(conserved_variables):
    density, flow_speed_vector, kinetic, thermodynamic_load = primitive(conserved_variables)
    return jnp.sqrt(2.0 * kinetic) + jnp.sqrt(GAMMA * thermodynamic_load / density)

def quantities(conserved_variables, sweep_coordinate):
    density, flow_speed_vector, kinetic, thermodynamic_load = primitive(conserved_variables)
    transported_scalar = flow_speed_vector[sweep_coordinate]
    interface_transport = [conserved_variables[0] * transported_scalar]
    for variable_index in range(3):
        tendency_increment = conserved_variables[1 + variable_index] * transported_scalar
        if variable_index == sweep_coordinate:
            tendency_increment = tendency_increment + thermodynamic_load
        interface_transport.append(tendency_increment)
    interface_transport.append((conserved_variables[4] + thermodynamic_load) * transported_scalar)
    return interface_transport + [flow_speed_vector[0], flow_speed_vector[1], flow_speed_vector[2], kinetic, thermodynamic_load / density]

def derivatives(section_terms, start_terms, along_axis, block, extent):
    position = jnp.arange(extent)
    home_block = position // block
    shape = [1, 1, 1]
    shape[along_axis] = extent
    inside = {}
    for offset in (1, 2, 3, 4, -1, -2, -3, -4):
        inside[offset] = ((position + offset) % extent // block == home_block).reshape(shape)

    def neighbour(variable_index, offset):
        current = jnp.roll(section_terms[variable_index], -offset, along_axis)
        if start_terms is None:
            return current
        earlier = jnp.roll(start_terms[variable_index], -offset, along_axis)
        return jnp.where(inside[offset], current, earlier)
    firsts = []
    seconds = []
    for variable_index in range(10):
        if variable_index < 5:
            result = jnp.zeros_like(section_terms[variable_index])
            for offset in range(4):
                result = result + FIRST[offset] * (neighbour(variable_index, offset + 1) - neighbour(variable_index, -offset - 1))
            firsts.append(result)
        else:
            result = CENTRE * section_terms[variable_index]
            for offset in range(4):
                result = result + SECOND[offset] * (neighbour(variable_index, offset + 1) + neighbour(variable_index, -offset - 1))
            seconds.append(result)
    return (firsts, seconds)

def assemble(parts):
    rate = []
    for variable_index in range(5):
        rate.append(-(parts[0][0][variable_index] + parts[1][0][variable_index] + parts[2][0][variable_index]))
    lap = [parts[0][1][variable_index] + parts[1][1][variable_index] + parts[2][1][variable_index] for variable_index in range(5)]
    rate[1] = rate[1] + VISCOSITY * lap[0]
    rate[2] = rate[2] + VISCOSITY * lap[1]
    rate[3] = rate[3] + VISCOSITY * lap[2]
    rate[4] = rate[4] + VISCOSITY * lap[3] + CONDUCTION * lap[4]
    return jnp.stack(rate, 0)

def reference(start_state, section_state, previous_speed):
    x_parts = derivatives(quantities(section_state, 0), quantities(start_state, 0), 0, CX, NX)
    y_parts = derivatives(quantities(section_state, 1), quantities(start_state, 1), 1, CY, NY)
    z_parts = derivatives(quantities(section_state, 2), None, 2, NZ, NZ)
    rate = assemble((x_parts, y_parts, z_parts))
    time_step = COURANT / previous_speed
    new_state = 0.75 * start_state + 0.25 * (section_state + time_step * rate)
    next_speed = jnp.max(wave_speed(new_state))
    return (new_state, next_speed)
```

```python
import functools

import jax
import jax.numpy as jnp
from jax import lax
from jax.experimental import pallas as pl
from jax.experimental.pallas import tpu as pltpu
from jax.sharding import PartitionSpec as P

GAMMA = 1.4
COURANT = 0.3
VISCOSITY = 0.05
CONDUCTION = 0.07
FIRST = (0.8, -0.2, 4.0 / 105.0, -1.0 / 280.0)
SECOND = (1.6, -0.2, 8.0 / 315.0, -1.0 / 560.0)
CENTRE = -205.0 / 72.0
WIDTH = 4
ROWS = 8
MESH = pl.DeviceIdType.MESH


def primitive(q):
    density, m1, m2, m3, energy = q
    inverse = 1.0 / density
    u, v, w = m1 * inverse, m2 * inverse, m3 * inverse
    kinetic = 0.5 * (u * u + v * v + w * w)
    pressure = (GAMMA - 1.0) * (energy - density * kinetic)
    return inverse, (u, v, w), kinetic, pressure


def wave_speed(q):
    inverse, _, kinetic, pressure = primitive(q)
    return jnp.sqrt(2.0 * kinetic) + jnp.sqrt(GAMMA * (pressure * inverse))


def smooth_terms(primitives):
    inverse, (u, v, w), kinetic, pressure = primitives
    return [
        VISCOSITY * u,
        VISCOSITY * v,
        VISCOSITY * w,
        VISCOSITY * kinetic + CONDUCTION * (pressure * inverse),
    ]


def flux_terms(q, primitives, direction):
    _, velocity, _, pressure = primitives
    speed = velocity[direction]
    flux = [q[1 + direction]]
    for k in range(3):
        term = q[1 + k] * speed
        flux.append(term + pressure if k == direction else term)
    flux.append((q[4] + pressure) * speed)
    return flux


def over_peers(devices, body, carry):
    if devices > 64:
        return lax.fori_loop(1, devices, body, carry)
    for k in range(1, devices):
        carry = body(k, carry)
    return carry


def meeting_rounds(nx, ny):
    rounds, known = [], 1
    while 2 * known < nx:
        rounds.append(("gx", known))
        known *= 2
    known = 0
    while 2 * known < ny:
        rounds.append(("gy", max(known, 1)))
        known = 2 * known if known else 1
    return rounds


def kernel(
    nx, ny, start, section, speed, out, next_speed,
    old, sec, acc, fx, fy, sm, xhalo, ylo, yhi, top, got,
    load_sem, xs_sem, xr_sem, ys_sem, yr_sem, ts_sem, tr_sem, meet_sem,
):
    _, cx, cy, nz = old.shape
    tiles = cy // ROWS
    devices = nx * ny
    me_x, me_y = lax.axis_index("gx"), lax.axis_index("gy")
    odd = lax.rem(me_x, 2)

    def on_x(k):
        return (lax.rem(me_x + k, nx), me_y)

    def on_y(k):
        return (me_x, lax.rem(me_y + k, ny))

    neighbours = (on_x(1), on_x(nx - 1), on_y(1), on_y(ny - 1))
    barrier = pltpu.get_barrier_semaphore()
    for device in neighbours:
        pl.semaphore_signal(barrier, inc=1, device_id=device, device_id_type=MESH)
    load_section = pltpu.make_async_copy(section, sec, load_sem.at[0])
    load_start = pltpu.make_async_copy(start, old, load_sem.at[1])
    load_start.start()
    load_section.start()

    def x_copy(turn, t):
        side = 1 - odd if turn == 0 else odd
        first = (1 - side) * (cx - WIDTH)
        return pltpu.make_async_remote_copy(
            src_ref=old.at[:, pl.ds(first, WIDTH), pl.ds(t * ROWS, ROWS), :],
            dst_ref=xhalo.at[side, t],
            send_sem=xs_sem.at[side, t],
            recv_sem=xr_sem.at[side, t],
            device_id=on_x(nx + 1 - 2 * side),
            device_id_type=MESH,
        )

    def x_arrival(turn, t):
        side = odd if turn == 0 else 1 - odd
        return side, pltpu.make_async_remote_copy(
            src_ref=old.at[:, pl.ds(0, WIDTH), pl.ds(t * ROWS, ROWS), :],
            dst_ref=xhalo.at[side, t],
            send_sem=xs_sem.at[side, t],
            recv_sem=xr_sem.at[side, t],
            device_id=on_x(1),
            device_id_type=MESH,
        )

    def y_copy(side):
        rows = pl.ds(cy - ROWS, ROWS) if side == 0 else pl.ds(0, ROWS)
        return pltpu.make_async_remote_copy(
            src_ref=old.at[:, :, rows, :],
            dst_ref=ylo if side == 0 else yhi,
            send_sem=ys_sem.at[side],
            recv_sem=yr_sem.at[side],
            device_id=on_y(1) if side == 0 else on_y(ny - 1),
            device_id_type=MESH,
        )

    load_start.wait()
    pl.semaphore_wait(barrier, 4)
    for turn in range(2):
        for t in range(tiles):
            x_copy(turn, t).start()
        if turn == 0:
            for side in range(2):
                y_copy(side).start()

    rounds = meeting_rounds(nx, ny)

    def meet(r):
        axis, distance = rounds[r]
        for k in (distance, -distance):
            device = on_x(nx + k) if axis == "gx" else on_y(ny + k)
            pl.semaphore_signal(meet_sem.at[r], inc=1, device_id=device, device_id_type=MESH)

    def met(r):
        pl.semaphore_wait(meet_sem.at[r], 2)
        if r + 1 < len(rounds):
            meet(r + 1)

    meet(0)

    scale = 0.25 * (COURANT / speed[0, 0])

    edge = jnp.zeros((WIDTH, cy, nz), jnp.float32)
    for c in range(5):
        fx[c, 0:WIDTH] = edge
        fx[c, cx + WIDTH : cx + 2 * WIDTH] = edge
    for c in range(4):
        sm[c, 0:WIDTH, ROWS : ROWS + cy] = edge
        sm[c, cx + WIDTH : cx + 2 * WIDTH, ROWS : ROWS + cy] = edge

    load_section.wait()

    def along_z(i, _):
        q = [sec[c, i] for c in range(5)]
        prim = primitive(q)
        smooth = smooth_terms(prim)
        for c, term in enumerate(flux_terms(q, prim, 0)):
            fx[c, i + WIDTH] = term
        for c, term in enumerate(flux_terms(q, prim, 1)):
            fy[c, i, ROWS : ROWS + cy] = term
        for c, term in enumerate(smooth):
            sm[c, i + WIDTH, ROWS : ROWS + cy] = term
        for c, term in enumerate(flux_terms(q, prim, 2)):
            total = None
            for m in range(1, WIDTH + 1):
                f = FIRST[m - 1] * term
                if c > 0:
                    s = SECOND[m - 1] * smooth[c - 1]
                    above, below = s - f, s + f
                else:
                    above, below = -f, f
                pair = pltpu.roll(above, nz - m, 1) + pltpu.roll(below, m, 1)
                total = pair if total is None else total + pair
            if c > 0:
                total = total + (3.0 * CENTRE) * smooth[c - 1]
            acc[c, i] = total
        return 0

    lax.fori_loop(0, cx, along_z, 0)
    met(0)

    def along_x(i, _):
        for c in range(5):
            total = acc[c, i]
            for m in range(1, WIDTH + 1):
                total = total - FIRST[m - 1] * (fx[c, i + WIDTH + m] - fx[c, i + WIDTH - m])
                if c > 0:
                    total = total + SECOND[m - 1] * (
                        sm[c - 1, i + WIDTH + m, ROWS : ROWS + cy]
                        + sm[c - 1, i + WIDTH - m, ROWS : ROWS + cy]
                    )
            acc[c, i] = total
        return 0

    lax.fori_loop(0, cx, along_x, 0)
    met(1)

    y_copy(0).wait_recv()
    y_copy(1).wait_recv()

    def along_y(i, _):
        for halo, first in ((ylo, 0), (yhi, ROWS + cy)):
            q = [halo[c, i] for c in range(5)]
            prim = primitive(q)
            for c, term in enumerate(flux_terms(q, prim, 1)):
                fy[c, i, first : first + ROWS] = term
            for c, term in enumerate(smooth_terms(prim)):
                sm[c, i + WIDTH, first : first + ROWS] = term
        for c in range(5):
            total = acc[c, i]
            for m in range(1, WIDTH + 1):
                above, below = ROWS + m, ROWS - m
                total = total - FIRST[m - 1] * (
                    fy[c, i, above : above + cy] - fy[c, i, below : below + cy]
                )
                if c > 0:
                    total = total + SECOND[m - 1] * (
                        sm[c - 1, i + WIDTH, above : above + cy]
                        + sm[c - 1, i + WIDTH, below : below + cy]
                    )
            acc[c, i] = total
        return 0

    lax.fori_loop(0, cx, along_y, 0)
    met(2)
    for r in range(3, len(rounds)):
        met(r)

    largest = None
    for turn in range(2):
        for t in range(tiles):
            rows = slice(t * ROWS, (t + 1) * ROWS)
            side, arrival = x_arrival(turn, t)
            arrival.wait_recv()
            sign = (1 - 2 * side).astype(jnp.float32)
            inner = [side * (cx - 1 - 2 * i) + i for i in range(WIDTH)]
            totals = [[acc[c, inner[i], rows] for c in range(5)] for i in range(WIDTH)]
            for h in range(WIDTH):
                q = [xhalo[side, t, c, side * (WIDTH - 1 - 2 * h) + h] for c in range(5)]
                prim = primitive(q)
                flux = [sign * f for f in flux_terms(q, prim, 0)]
                smooth = smooth_terms(prim)
                for i in range(h + 1):
                    m = i + WIDTH - h
                    for c in range(5):
                        term = FIRST[m - 1] * flux[c]
                        if c > 0:
                            term = term + SECOND[m - 1] * smooth[c - 1]
                        totals[i][c] = totals[i][c] + term
            for i in range(WIDTH):
                new = []
                for c in range(5):
                    value = (
                        0.75 * old[c, inner[i], rows]
                        + 0.25 * sec[c, inner[i], rows]
                        + scale * totals[i][c]
                    )
                    out[c, inner[i], rows] = value
                    new.append(value)
                wave = wave_speed(new)
                largest = wave if largest is None else jnp.maximum(largest, wave)

    def top_copy(k):
        return pltpu.make_async_remote_copy(
            src_ref=top,
            dst_ref=got.at[k],
            send_sem=ts_sem.at[k],
            recv_sem=tr_sem.at[k],
            device_id=(lax.rem(me_x + k // ny, nx), lax.rem(me_y + k % ny, ny)),
            device_id_type=MESH,
        )

    folded = largest[:, 0:128]
    for first in range(128, nz, 128):
        folded = jnp.maximum(folded, largest[:, first : first + 128])
    peak = jnp.max(folded, axis=0, keepdims=True)
    top[...] = peak

    def send(k, _):
        top_copy(k).start()
        return 0

    over_peers(devices, send, 0)
    for turn in range(2):
        for t in range(tiles):
            x_copy(turn, t).wait_send()
    for side in range(2):
        y_copy(side).wait_send()

    def receive(k, peak):
        top_copy(k).wait_recv()
        return jnp.maximum(peak, got[k])

    peak = over_peers(devices, receive, peak)
    next_speed[...] = jnp.broadcast_to(jnp.max(peak, axis=1, keepdims=True), next_speed.shape)

    def sent(k, _):
        top_copy(k).wait_send()
        return 0

    over_peers(devices, sent, 0)


def finish(state, peak, new_state, next_speed, sem):
    comps = state.shape[0]
    copies = [
        pltpu.make_async_copy(state.at[c], new_state.at[c], sem.at[c]) for c in range(comps)
    ]
    copies.append(pltpu.make_async_copy(peak, next_speed, sem.at[comps]))
    for copy in copies:
        copy.start()
    for copy in copies:
        copy.wait()


def local(nx, ny, start_state, section_state, previous_speed):
    comps, cx, cy, nz = section_state.shape
    tiles = cy // ROWS
    f32 = jnp.float32
    dma = pltpu.SemaphoreType.DMA
    state, peak = pl.pallas_call(
        functools.partial(kernel, nx, ny),
        out_shape=(
            pltpu.VMEM(section_state.shape, f32),
            pltpu.VMEM((1, 128), f32),
        ),
        in_specs=[
            pl.BlockSpec(memory_space=pl.ANY),
            pl.BlockSpec(memory_space=pl.ANY),
            pl.BlockSpec(memory_space=pltpu.SMEM),
        ],
        out_specs=(
            pl.BlockSpec(memory_space=pltpu.VMEM),
            pl.BlockSpec(memory_space=pltpu.VMEM),
        ),
        scratch_shapes=[
            pltpu.VMEM(section_state.shape, f32),
            pltpu.VMEM(section_state.shape, f32),
            pltpu.VMEM(section_state.shape, f32),
            pltpu.VMEM((comps, cx + 2 * WIDTH, cy, nz), f32),
            pltpu.VMEM((comps, cx, cy + 2 * ROWS, nz), f32),
            pltpu.VMEM((comps - 1, cx + 2 * WIDTH, cy + 2 * ROWS, nz), f32),
            pltpu.VMEM((2, tiles, comps, WIDTH, ROWS, nz), f32),
            pltpu.VMEM((comps, cx, ROWS, nz), f32),
            pltpu.VMEM((comps, cx, ROWS, nz), f32),
            pltpu.VMEM((1, 128), f32),
            pltpu.VMEM((nx * ny, 1, 128), f32),
            dma((2,)),
            dma((2, tiles)),
            dma((2, tiles)),
            dma((2,)),
            dma((2,)),
            dma((nx * ny,)),
            dma((nx * ny,)),
            pltpu.SemaphoreType.REGULAR((len(meeting_rounds(nx, ny)),)),
        ],
        compiler_params=pltpu.CompilerParams(collective_id=0, has_side_effects=True),
        name="section_step",
    )(start_state, section_state, previous_speed.reshape(1, 1))
    new_state, next_speed = pl.pallas_call(
        finish,
        out_shape=(
            jax.ShapeDtypeStruct(section_state.shape, f32),
            jax.ShapeDtypeStruct((1, 128), f32),
        ),
        in_specs=[pl.BlockSpec(memory_space=pltpu.VMEM)] * 2,
        out_specs=(pl.BlockSpec(memory_space=pl.ANY), pl.BlockSpec(memory_space=pl.ANY)),
        scratch_shapes=[dma((comps + 1,))],
        name="write_out",
    )(
        pltpu.with_memory_space_constraint(state, pltpu.VMEM),
        pltpu.with_memory_space_constraint(peak, pltpu.VMEM),
    )
    return new_state, next_speed[0, 0]


def solution(mesh):
    nx, ny = mesh.shape["gx"], mesh.shape["gy"]
    in_specs = (P(None, "gx", "gy", None), P(None, "gx", "gy", None), P())
    out_specs = (P(None, "gx", "gy", None), P())
    return jax.shard_map(
        functools.partial(local, nx, ny),
        mesh=mesh,
        in_specs=in_specs,
        out_specs=out_specs,
        check_vma=False,
    )
```

```python
import functools

import jax
import jax.numpy as jnp
from jax import lax
from jax.experimental import pallas as pl
from jax.experimental.pallas import tpu as pltpu
from jax.sharding import PartitionSpec as P

GAMMA = 1.4
COURANT = 0.3
VISCOSITY = 0.05
CONDUCTION = 0.07
FIRST = (0.8, -0.2, 4.0 / 105.0, -1.0 / 280.0)
SECOND = (1.6, -0.2, 8.0 / 315.0, -1.0 / 560.0)
CENTRE = -205.0 / 72.0
WIDTH = 4
ROWS = 8
DETOUR = 1
MESH = pl.DeviceIdType.MESH


def primitive(q):
    density, m1, m2, m3, energy = q
    inverse = 1.0 / density
    u, v, w = m1 * inverse, m2 * inverse, m3 * inverse
    kinetic = 0.5 * (u * u + v * v + w * w)
    pressure = (GAMMA - 1.0) * (energy - density * kinetic)
    return inverse, (u, v, w), kinetic, pressure


def wave_speed(q):
    inverse, _, kinetic, pressure = primitive(q)
    return jnp.sqrt(2.0 * kinetic) + jnp.sqrt(GAMMA * (pressure * inverse))


def smooth_terms(primitives):
    inverse, (u, v, w), kinetic, pressure = primitives
    return [
        VISCOSITY * u,
        VISCOSITY * v,
        VISCOSITY * w,
        VISCOSITY * kinetic + CONDUCTION * (pressure * inverse),
    ]


def flux_terms(q, primitives, direction):
    _, velocity, _, pressure = primitives
    speed = velocity[direction]
    flux = [q[1 + direction]]
    for k in range(3):
        term = q[1 + k] * speed
        flux.append(term + pressure if k == direction else term)
    flux.append((q[4] + pressure) * speed)
    return flux


def over_peers(devices, body, carry):
    if devices > 64:
        return lax.fori_loop(1, devices, body, carry)
    for k in range(1, devices):
        carry = body(k, carry)
    return carry


def meeting_rounds(nx, ny):
    rounds, known = [], 1
    while 2 * known < nx:
        rounds.append(("gx", known))
        known *= 2
    known = 0
    while 2 * known < ny:
        rounds.append(("gy", max(known, 1)))
        known = 2 * known if known else 1
    return rounds


def kernel(
    nx, ny, start, section, speed, out, next_speed,
    old, sec, acc, fx, fy, sm, xhalo, relay, ylo, yhi, top, got,
    load_sem, ns_sem, nr_sem, fs_sem, fr_sem, ds_sem, dr_sem, rr_sem, rs_sem,
    ys_sem, yr_sem, ts_sem, tr_sem, meet_sem, ring_sem,
):
    _, cx, cy, nz = old.shape
    tiles = cy // ROWS
    devices = nx * ny
    me_x, me_y = lax.axis_index("gx"), lax.axis_index("gy")
    odd = lax.rem(me_x, 2)

    def on_x(k):
        return (lax.rem(me_x + k, nx), me_y)

    def on_y(k):
        return (me_x, lax.rem(me_y + k, ny))

    first, last = me_x == 0, me_x == nx - 1
    near, far = on_x(nx + 1 - 2 * odd), on_x(nx - 1 + 2 * odd)
    beyond = on_x(nx + 2 - 4 * odd)
    detours = first | ((odd == 1) & (me_x < nx - 1))
    carries = (me_x == 1) | ((odd == 0) & (me_x < nx - 2))

    barrier = pltpu.get_barrier_semaphore()

    def greet(device, sem=barrier):
        pl.semaphore_signal(sem, inc=1, device_id=device, device_id_type=MESH)

    for device in (near, on_y(1), on_y(ny - 1)):
        greet(device)

    @pl.when(jnp.logical_not(first | last))
    def _():
        greet(far)

    @pl.when((odd == 0) & (me_x > 0))
    def _():
        greet(on_x(nx - 2))

    load_section = pltpu.make_async_copy(section, sec, load_sem.at[0])
    load_start = pltpu.make_async_copy(start, old, load_sem.at[1])
    load_start.start()
    load_section.start()

    direct = old.shape[0] - DETOUR

    def remote(src, dst, send_sem, recv_sem, device):
        return pltpu.make_async_remote_copy(
            src_ref=src,
            dst_ref=dst,
            send_sem=send_sem,
            recv_sem=recv_sem,
            device_id=device,
            device_id_type=MESH,
        )

    def edge_of(side, t, comps):
        return old.at[comps, pl.ds((1 - side) * (cx - WIDTH), WIDTH), pl.ds(t * ROWS, ROWS), :]

    def near_copy(t, side):
        every = pl.ds(0, old.shape[0])
        return remote(edge_of(odd, t, every), xhalo.at[side, t], ns_sem.at[t], nr_sem.at[t], near)

    def far_copy(t, side):
        some = pl.ds(0, direct)
        return remote(
            edge_of(1 - odd, t, some), xhalo.at[side, t, some], fs_sem.at[t], fr_sem.at[t], far
        )

    def rest_copy(t, side):
        rest = pl.ds(direct, DETOUR)
        return remote(
            edge_of(1 - odd, t, rest), xhalo.at[side, t, rest], ds_sem.at[t], dr_sem.at[t], far
        )

    def detour_copy(t):
        rest = pl.ds(direct, DETOUR)
        return remote(edge_of(1 - odd, t, rest), relay.at[t], ds_sem.at[t], rr_sem.at[t], near)

    def carry_copy(t):
        rest = pl.ds(direct, DETOUR)
        return remote(
            relay.at[t], xhalo.at[odd, t, rest], rs_sem.at[t], dr_sem.at[t], beyond
        )

    def y_copy(side):
        rows = pl.ds(cy - ROWS, ROWS) if side == 0 else pl.ds(0, ROWS)
        return pltpu.make_async_remote_copy(
            src_ref=old.at[:, :, rows, :],
            dst_ref=ylo if side == 0 else yhi,
            send_sem=ys_sem.at[side],
            recv_sem=yr_sem.at[side],
            device_id=on_y(1) if side == 0 else on_y(ny - 1),
            device_id_type=MESH,
        )

    def start_far():
        for t in range(tiles):
            far_copy(t, 1 - odd).start()

        @pl.when(jnp.logical_not(detours))
        def _():
            for t in range(tiles):
                rest_copy(t, 1 - odd).start()

    load_start.wait()
    carried = jnp.where((odd == 0) & (me_x < nx - 2), 1, 0)
    pl.semaphore_wait(barrier, jnp.where(first, 3, 4) + carried)

    @pl.when(first)
    def _():
        greet(far)

    @pl.when(last)
    def _():
        greet(far, ring_sem)
        greet(on_x(2), ring_sem)

    @pl.when(detours)
    def _():
        for t in range(tiles):
            detour_copy(t).start()

    @pl.when(jnp.logical_not(first))
    def _():
        start_far()

    for t in range(tiles):
        near_copy(t, odd).start()
    for side in range(2):
        y_copy(side).start()

    rounds = meeting_rounds(nx, ny)

    def meet(r):
        axis, distance = rounds[r]
        for k in (distance, -distance):
            device = on_x(nx + k) if axis == "gx" else on_y(ny + k)
            pl.semaphore_signal(meet_sem.at[r], inc=1, device_id=device, device_id_type=MESH)

    def met(r):
        pl.semaphore_wait(meet_sem.at[r], 2)
        if r + 1 < len(rounds):
            meet(r + 1)

    scale = 0.25 * (COURANT / speed[0, 0])

    edge = jnp.zeros((WIDTH, cy, nz), jnp.float32)
    for c in range(5):
        fx[c, 0:WIDTH] = edge
        fx[c, cx + WIDTH : cx + 2 * WIDTH] = edge
    for c in range(4):
        sm[c, 0:WIDTH, ROWS : ROWS + cy] = edge
        sm[c, cx + WIDTH : cx + 2 * WIDTH, ROWS : ROWS + cy] = edge

    load_section.wait()

    def along_z(i, _):
        q = [sec[c, i] for c in range(5)]
        prim = primitive(q)
        smooth = smooth_terms(prim)
        for c, term in enumerate(flux_terms(q, prim, 0)):
            fx[c, i + WIDTH] = term
        for c, term in enumerate(flux_terms(q, prim, 1)):
            fy[c, i, ROWS : ROWS + cy] = term
        for c, term in enumerate(smooth):
            sm[c, i + WIDTH, ROWS : ROWS + cy] = term
        for c, term in enumerate(flux_terms(q, prim, 2)):
            total = None
            for m in range(1, WIDTH + 1):
                f = FIRST[m - 1] * term
                if c > 0:
                    s = SECOND[m - 1] * smooth[c - 1]
                    above, below = s - f, s + f
                else:
                    above, below = -f, f
                pair = pltpu.roll(above, nz - m, 1) + pltpu.roll(below, m, 1)
                total = pair if total is None else total + pair
            if c > 0:
                total = total + (3.0 * CENTRE) * smooth[c - 1]
            acc[c, i] = total
        return 0

    lax.fori_loop(0, cx, along_z, 0)

    @pl.when(first | (me_x == 1))
    def _():
        pl.semaphore_wait(ring_sem, 1)

    @pl.when(first)
    def _():
        start_far()

    @pl.when(carries)
    def _():
        for t in range(tiles):
            detour_copy(t).wait_recv()
            carry_copy(t).start()

    meet(0)

    def along_x(i, _):
        for c in range(5):
            total = acc[c, i]
            for m in range(1, WIDTH + 1):
                total = total - FIRST[m - 1] * (fx[c, i + WIDTH + m] - fx[c, i + WIDTH - m])
                if c > 0:
                    total = total + SECOND[m - 1] * (
                        sm[c - 1, i + WIDTH + m, ROWS : ROWS + cy]
                        + sm[c - 1, i + WIDTH - m, ROWS : ROWS + cy]
                    )
            acc[c, i] = total
        return 0

    lax.fori_loop(0, cx, along_x, 0)
    met(0)
    met(1)

    y_copy(0).wait_recv()
    y_copy(1).wait_recv()

    def along_y(i, _):
        for halo, first in ((ylo, 0), (yhi, ROWS + cy)):
            q = [halo[c, i] for c in range(5)]
            prim = primitive(q)
            for c, term in enumerate(flux_terms(q, prim, 1)):
                fy[c, i, first : first + ROWS] = term
            for c, term in enumerate(smooth_terms(prim)):
                sm[c, i + WIDTH, first : first + ROWS] = term
        for c in range(5):
            total = acc[c, i]
            for m in range(1, WIDTH + 1):
                above, below = ROWS + m, ROWS - m
                total = total - FIRST[m - 1] * (
                    fy[c, i, above : above + cy] - fy[c, i, below : below + cy]
                )
                if c > 0:
                    total = total + SECOND[m - 1] * (
                        sm[c - 1, i + WIDTH, above : above + cy]
                        + sm[c - 1, i + WIDTH, below : below + cy]
                    )
            acc[c, i] = total
        return 0

    lax.fori_loop(0, cx, along_y, 0)
    met(2)
    for r in range(3, len(rounds)):
        met(r)

    largest = None
    for t in range(tiles):
        for turn in range(2):
            rows = slice(t * ROWS, (t + 1) * ROWS)
            if turn == 0:
                side = odd
                far_copy(t, side).wait_recv()
                rest_copy(t, side).wait_recv()
            else:
                side = 1 - odd
                near_copy(t, side).wait_recv()
            sign = (1 - 2 * side).astype(jnp.float32)
            inner = [side * (cx - 1 - 2 * i) + i for i in range(WIDTH)]
            totals = [[acc[c, inner[i], rows] for c in range(5)] for i in range(WIDTH)]
            for h in range(WIDTH):
                q = [xhalo[side, t, c, side * (WIDTH - 1 - 2 * h) + h] for c in range(5)]
                prim = primitive(q)
                flux = [sign * f for f in flux_terms(q, prim, 0)]
                smooth = smooth_terms(prim)
                for i in range(h + 1):
                    m = i + WIDTH - h
                    for c in range(5):
                        term = FIRST[m - 1] * flux[c]
                        if c > 0:
                            term = term + SECOND[m - 1] * smooth[c - 1]
                        totals[i][c] = totals[i][c] + term
            for i in range(WIDTH):
                new = []
                for c in range(5):
                    value = (
                        0.75 * old[c, inner[i], rows]
                        + 0.25 * sec[c, inner[i], rows]
                        + scale * totals[i][c]
                    )
                    out[c, inner[i], rows] = value
                    new.append(value)
                wave = wave_speed(new)
                largest = wave if largest is None else jnp.maximum(largest, wave)

    def top_copy(k):
        return pltpu.make_async_remote_copy(
            src_ref=top,
            dst_ref=got.at[k],
            send_sem=ts_sem.at[k],
            recv_sem=tr_sem.at[k],
            device_id=(lax.rem(me_x + k // ny, nx), lax.rem(me_y + k % ny, ny)),
            device_id_type=MESH,
        )

    folded = largest[:, 0:128]
    for first in range(128, nz, 128):
        folded = jnp.maximum(folded, largest[:, first : first + 128])
    peak = jnp.max(folded, axis=0, keepdims=True)
    top[...] = peak

    def send(k, _):
        top_copy(k).start()
        return 0

    over_peers(devices, send, 0)
    for t in range(tiles):
        near_copy(t, odd).wait_send()
        far_copy(t, 1 - odd).wait_send()
        rest_copy(t, 1 - odd).wait_send()

    @pl.when(carries)
    def _():
        for t in range(tiles):
            carry_copy(t).wait_send()

    for side in range(2):
        y_copy(side).wait_send()

    def receive(k, peak):
        top_copy(k).wait_recv()
        return jnp.maximum(peak, got[k])

    peak = over_peers(devices, receive, peak)
    next_speed[...] = jnp.broadcast_to(jnp.max(peak, axis=1, keepdims=True), next_speed.shape)

    def sent(k, _):
        top_copy(k).wait_send()
        return 0

    over_peers(devices, sent, 0)


def finish(state, peak, new_state, next_speed, sem):
    comps = state.shape[0]
    copies = [
        pltpu.make_async_copy(state.at[c], new_state.at[c], sem.at[c]) for c in range(comps)
    ]
    copies.append(pltpu.make_async_copy(peak, next_speed, sem.at[comps]))
    for copy in copies:
        copy.start()
    for copy in copies:
        copy.wait()


def local(nx, ny, start_state, section_state, previous_speed):
    comps, cx, cy, nz = section_state.shape
    tiles = cy // ROWS
    f32 = jnp.float32
    dma = pltpu.SemaphoreType.DMA
    state, peak = pl.pallas_call(
        functools.partial(kernel, nx, ny),
        out_shape=(
            pltpu.VMEM(section_state.shape, f32),
            pltpu.VMEM((1, 128), f32),
        ),
        in_specs=[
            pl.BlockSpec(memory_space=pl.ANY),
            pl.BlockSpec(memory_space=pl.ANY),
            pl.BlockSpec(memory_space=pltpu.SMEM),
        ],
        out_specs=(
            pl.BlockSpec(memory_space=pltpu.VMEM),
            pl.BlockSpec(memory_space=pltpu.VMEM),
        ),
        scratch_shapes=[
            pltpu.VMEM(section_state.shape, f32),
            pltpu.VMEM(section_state.shape, f32),
            pltpu.VMEM(section_state.shape, f32),
            pltpu.VMEM((comps, cx + 2 * WIDTH, cy, nz), f32),
            pltpu.VMEM((comps, cx, cy + 2 * ROWS, nz), f32),
            pltpu.VMEM((comps - 1, cx + 2 * WIDTH, cy + 2 * ROWS, nz), f32),
            pltpu.VMEM((2, tiles, comps, WIDTH, ROWS, nz), f32),
            pltpu.VMEM((tiles, DETOUR, WIDTH, ROWS, nz), f32),
            pltpu.VMEM((comps, cx, ROWS, nz), f32),
            pltpu.VMEM((comps, cx, ROWS, nz), f32),
            pltpu.VMEM((1, 128), f32),
            pltpu.VMEM((nx * ny, 1, 128), f32),
            dma((2,)),
            dma((tiles,)),
            dma((tiles,)),
            dma((tiles,)),
            dma((tiles,)),
            dma((tiles,)),
            dma((tiles,)),
            dma((tiles,)),
            dma((tiles,)),
            dma((2,)),
            dma((2,)),
            dma((nx * ny,)),
            dma((nx * ny,)),
            pltpu.SemaphoreType.REGULAR((len(meeting_rounds(nx, ny)),)),
            pltpu.SemaphoreType.REGULAR,
        ],
        compiler_params=pltpu.CompilerParams(collective_id=0, has_side_effects=True),
        name="section_step",
    )(start_state, section_state, previous_speed.reshape(1, 1))
    new_state, next_speed = pl.pallas_call(
        finish,
        out_shape=(
            jax.ShapeDtypeStruct(section_state.shape, f32),
            jax.ShapeDtypeStruct((1, 128), f32),
        ),
        in_specs=[pl.BlockSpec(memory_space=pltpu.VMEM)] * 2,
        out_specs=(pl.BlockSpec(memory_space=pl.ANY), pl.BlockSpec(memory_space=pl.ANY)),
        scratch_shapes=[dma((comps + 1,))],
        name="write_out",
    )(
        pltpu.with_memory_space_constraint(state, pltpu.VMEM),
        pltpu.with_memory_space_constraint(peak, pltpu.VMEM),
    )
    return new_state, next_speed[0, 0]


def solution(mesh):
    nx, ny = mesh.shape["gx"], mesh.shape["gy"]
    in_specs = (P(None, "gx", "gy", None), P(None, "gx", "gy", None), P())
    out_specs = (P(None, "gx", "gy", None), P())
    return jax.shard_map(
        functools.partial(local, nx, ny),
        mesh=mesh,
        in_specs=in_specs,
        out_specs=out_specs,
        check_vma=False,
    )
```

```python
import functools

import jax
import jax.numpy as jnp
from jax import lax
from jax.experimental import pallas as pl
from jax.experimental.pallas import tpu as pltpu
from jax.sharding import PartitionSpec as P

GAMMA = 1.4
COURANT = 0.3
VISCOSITY = 0.05
CONDUCTION = 0.07
FIRST = (0.8, -0.2, 4.0 / 105.0, -1.0 / 280.0)
SECOND = (1.6, -0.2, 8.0 / 315.0, -1.0 / 560.0)
CENTRE = -205.0 / 72.0
WIDTH = 4
ROWS = 8
DETOUR = 1
MESH = pl.DeviceIdType.MESH


def primitive(q):
    density, m1, m2, m3, energy = q
    inverse = 1.0 / density
    u, v, w = m1 * inverse, m2 * inverse, m3 * inverse
    kinetic = 0.5 * (u * u + v * v + w * w)
    pressure = (GAMMA - 1.0) * (energy - density * kinetic)
    return inverse, (u, v, w), kinetic, pressure


def wave_speed(q):
    inverse, _, kinetic, pressure = primitive(q)
    return jnp.sqrt(2.0 * kinetic) + jnp.sqrt(GAMMA * (pressure * inverse))


def smooth_terms(primitives):
    inverse, (u, v, w), kinetic, pressure = primitives
    return [
        VISCOSITY * u,
        VISCOSITY * v,
        VISCOSITY * w,
        VISCOSITY * kinetic + CONDUCTION * (pressure * inverse),
    ]


def flux_terms(q, primitives, direction):
    _, velocity, _, pressure = primitives
    speed = velocity[direction]
    flux = [q[1 + direction]]
    for k in range(3):
        term = q[1 + k] * speed
        flux.append(term + pressure if k == direction else term)
    flux.append((q[4] + pressure) * speed)
    return flux


def meeting_rounds(nx, ny):
    rounds, known = [], 1
    while 2 * known < nx:
        rounds.append(("gx", known))
        known *= 2
    known = 0
    while 2 * known < ny:
        rounds.append(("gy", max(known, 1)))
        known = 2 * known if known else 1
    return rounds


def kernel(
    nx, ny, start, section, speed, out, next_speed,
    old, sec, acc, fx, fy, sm, xhalo, relay, ylo, yhi, top, got,
    load_sem, ns_sem, nr_sem, fs_sem, fr_sem, ds_sem, dr_sem, rr_sem, rs_sem,
    ys_sem, yr_sem, ts_sem, tr_sem, meet_sem, ring_sem,
):
    _, cx, cy, nz = old.shape
    tiles = cy // ROWS
    devices = nx * ny
    me_x, me_y = lax.axis_index("gx"), lax.axis_index("gy")
    odd = lax.rem(me_x, 2)

    def on_x(k):
        return (lax.rem(me_x + k, nx), me_y)

    def on_y(k):
        return (me_x, lax.rem(me_y + k, ny))

    first, last = me_x == 0, me_x == nx - 1
    near, far = on_x(nx + 1 - 2 * odd), on_x(nx - 1 + 2 * odd)
    beyond = on_x(nx + 2 - 4 * odd)
    detours = first | ((odd == 1) & (me_x < nx - 1))
    carries = (me_x == 1) | ((odd == 0) & (me_x < nx - 2))

    barrier = pltpu.get_barrier_semaphore()

    def greet(device, sem=barrier):
        pl.semaphore_signal(sem, inc=1, device_id=device, device_id_type=MESH)

    for device in (near, on_y(1), on_y(ny - 1)):
        greet(device)

    @pl.when(jnp.logical_not(first | last))
    def _():
        greet(far)

    @pl.when((odd == 0) & (me_x > 0))
    def _():
        greet(on_x(nx - 2))

    load_section = pltpu.make_async_copy(section, sec, load_sem.at[0])
    load_start = pltpu.make_async_copy(start, old, load_sem.at[1])
    load_start.start()
    load_section.start()

    direct = old.shape[0] - DETOUR

    def remote(src, dst, send_sem, recv_sem, device):
        return pltpu.make_async_remote_copy(
            src_ref=src,
            dst_ref=dst,
            send_sem=send_sem,
            recv_sem=recv_sem,
            device_id=device,
            device_id_type=MESH,
        )

    def edge_of(side, t, comps):
        return old.at[comps, pl.ds((1 - side) * (cx - WIDTH), WIDTH), pl.ds(t * ROWS, ROWS), :]

    def near_copy(t, side):
        every = pl.ds(0, old.shape[0])
        return remote(edge_of(odd, t, every), xhalo.at[side, t], ns_sem.at[t], nr_sem.at[t], near)

    def far_copy(t, side):
        some = pl.ds(0, direct)
        return remote(
            edge_of(1 - odd, t, some), xhalo.at[side, t, some], fs_sem.at[t], fr_sem.at[t], far
        )

    def rest_copy(t, side):
        rest = pl.ds(direct, DETOUR)
        return remote(
            edge_of(1 - odd, t, rest), xhalo.at[side, t, rest], ds_sem.at[t], dr_sem.at[t], far
        )

    def detour_copy(t):
        rest = pl.ds(direct, DETOUR)
        return remote(edge_of(1 - odd, t, rest), relay.at[t], ds_sem.at[t], rr_sem.at[t], near)

    def carry_copy(t):
        rest = pl.ds(direct, DETOUR)
        return remote(
            relay.at[t], xhalo.at[odd, t, rest], rs_sem.at[t], dr_sem.at[t], beyond
        )

    def y_copy(side):
        rows = pl.ds(cy - ROWS, ROWS) if side == 0 else pl.ds(0, ROWS)
        return pltpu.make_async_remote_copy(
            src_ref=old.at[:, :, rows, :],
            dst_ref=ylo if side == 0 else yhi,
            send_sem=ys_sem.at[side],
            recv_sem=yr_sem.at[side],
            device_id=on_y(1) if side == 0 else on_y(ny - 1),
            device_id_type=MESH,
        )

    def start_far():
        for t in range(tiles):
            far_copy(t, 1 - odd).start()

        @pl.when(jnp.logical_not(detours))
        def _():
            for t in range(tiles):
                rest_copy(t, 1 - odd).start()

    load_start.wait()
    carried = jnp.where((odd == 0) & (me_x < nx - 2), 1, 0)
    pl.semaphore_wait(barrier, jnp.where(first, 3, 4) + carried)

    @pl.when(first)
    def _():
        greet(far)

    @pl.when(last)
    def _():
        greet(far, ring_sem)
        greet(on_x(2), ring_sem)

    @pl.when(detours)
    def _():
        for t in range(tiles):
            detour_copy(t).start()

    @pl.when(jnp.logical_not(first))
    def _():
        start_far()

    for t in range(tiles):
        near_copy(t, odd).start()
    for side in range(2):
        y_copy(side).start()

    rounds = meeting_rounds(nx, ny)

    def meet(r):
        axis, distance = rounds[r]
        for k in (distance, -distance):
            device = on_x(nx + k) if axis == "gx" else on_y(ny + k)
            pl.semaphore_signal(meet_sem.at[r], inc=1, device_id=device, device_id_type=MESH)

    def met(r):
        pl.semaphore_wait(meet_sem.at[r], 2)
        if r + 1 < len(rounds):
            meet(r + 1)

    scale = 0.25 * (COURANT / speed[0, 0])

    edge = jnp.zeros((WIDTH, cy, nz), jnp.float32)
    for c in range(5):
        fx[c, 0:WIDTH] = edge
        fx[c, cx + WIDTH : cx + 2 * WIDTH] = edge
    for c in range(4):
        sm[c, 0:WIDTH, ROWS : ROWS + cy] = edge
        sm[c, cx + WIDTH : cx + 2 * WIDTH, ROWS : ROWS + cy] = edge

    load_section.wait()

    def along_z(i, _):
        q = [sec[c, i] for c in range(5)]
        prim = primitive(q)
        smooth = smooth_terms(prim)
        for c, term in enumerate(flux_terms(q, prim, 0)):
            fx[c, i + WIDTH] = term
        for c, term in enumerate(flux_terms(q, prim, 1)):
            fy[c, i, ROWS : ROWS + cy] = term
        for c, term in enumerate(smooth):
            sm[c, i + WIDTH, ROWS : ROWS + cy] = term
        for c, term in enumerate(flux_terms(q, prim, 2)):
            total = None
            for m in range(1, WIDTH + 1):
                f = FIRST[m - 1] * term
                if c > 0:
                    s = SECOND[m - 1] * smooth[c - 1]
                    above, below = s - f, s + f
                else:
                    above, below = -f, f
                pair = pltpu.roll(above, nz - m, 1) + pltpu.roll(below, m, 1)
                total = pair if total is None else total + pair
            if c > 0:
                total = total + (3.0 * CENTRE) * smooth[c - 1]
            acc[c, i] = total
        return 0

    lax.fori_loop(0, cx, along_z, 0)

    @pl.when(first | (me_x == 1))
    def _():
        pl.semaphore_wait(ring_sem, 1)

    @pl.when(first)
    def _():
        start_far()

    @pl.when(carries)
    def _():
        for t in range(tiles):
            detour_copy(t).wait_recv()
            carry_copy(t).start()

    meet(0)

    def along_x(i, _):
        for c in range(5):
            total = acc[c, i]
            for m in range(1, WIDTH + 1):
                total = total - FIRST[m - 1] * (fx[c, i + WIDTH + m] - fx[c, i + WIDTH - m])
                if c > 0:
                    total = total + SECOND[m - 1] * (
                        sm[c - 1, i + WIDTH + m, ROWS : ROWS + cy]
                        + sm[c - 1, i + WIDTH - m, ROWS : ROWS + cy]
                    )
            acc[c, i] = total
        return 0

    lax.fori_loop(0, cx, along_x, 0)
    met(0)
    met(1)

    y_copy(0).wait_recv()
    y_copy(1).wait_recv()

    def along_y(i, _):
        for halo, first in ((ylo, 0), (yhi, ROWS + cy)):
            q = [halo[c, i] for c in range(5)]
            prim = primitive(q)
            for c, term in enumerate(flux_terms(q, prim, 1)):
                fy[c, i, first : first + ROWS] = term
            for c, term in enumerate(smooth_terms(prim)):
                sm[c, i + WIDTH, first : first + ROWS] = term
        for c in range(5):
            total = acc[c, i]
            for m in range(1, WIDTH + 1):
                above, below = ROWS + m, ROWS - m
                total = total - FIRST[m - 1] * (
                    fy[c, i, above : above + cy] - fy[c, i, below : below + cy]
                )
                if c > 0:
                    total = total + SECOND[m - 1] * (
                        sm[c - 1, i + WIDTH, above : above + cy]
                        + sm[c - 1, i + WIDTH, below : below + cy]
                    )
            acc[c, i] = total
        return 0

    lax.fori_loop(0, cx, along_y, 0)
    met(2)
    for r in range(3, len(rounds)):
        met(r)

    largest = None
    for t in range(tiles):
        for turn in range(2):
            rows = slice(t * ROWS, (t + 1) * ROWS)
            if turn == 0:
                side = odd
                far_copy(t, side).wait_recv()
                rest_copy(t, side).wait_recv()
            else:
                side = 1 - odd
                near_copy(t, side).wait_recv()
            sign = (1 - 2 * side).astype(jnp.float32)
            inner = [side * (cx - 1 - 2 * i) + i for i in range(WIDTH)]
            totals = [[acc[c, inner[i], rows] for c in range(5)] for i in range(WIDTH)]
            for h in range(WIDTH):
                q = [xhalo[side, t, c, side * (WIDTH - 1 - 2 * h) + h] for c in range(5)]
                prim = primitive(q)
                flux = [sign * f for f in flux_terms(q, prim, 0)]
                smooth = smooth_terms(prim)
                for i in range(h + 1):
                    m = i + WIDTH - h
                    for c in range(5):
                        term = FIRST[m - 1] * flux[c]
                        if c > 0:
                            term = term + SECOND[m - 1] * smooth[c - 1]
                        totals[i][c] = totals[i][c] + term
            for i in range(WIDTH):
                new = []
                for c in range(5):
                    value = (
                        0.75 * old[c, inner[i], rows]
                        + 0.25 * sec[c, inner[i], rows]
                        + scale * totals[i][c]
                    )
                    out[c, inner[i], rows] = value
                    new.append(value)
                wave = wave_speed(new)
                largest = wave if largest is None else jnp.maximum(largest, wave)

    me = me_x * ny + me_y

    def top_copy(k):
        to = k + (k >= me).astype(jnp.int32)
        return remote(top, got.at[me], ts_sem, tr_sem, (to // ny, lax.rem(to, ny)))

    def every_top():
        others = pl.ds(0, devices - 1)
        return remote(got.at[others], got.at[others], ts_sem, tr_sem, near)

    folded = largest[:, 0:128]
    for first in range(128, nz, 128):
        folded = jnp.maximum(folded, largest[:, first : first + 128])
    peak = jnp.max(folded, axis=0, keepdims=True)
    top[...] = peak

    def send(k, _):
        top_copy(k).start()
        return 0

    lax.fori_loop(0, devices - 1, send, 0, unroll=devices <= 64)
    got[me] = peak
    for t in range(tiles):
        near_copy(t, odd).wait_send()
        far_copy(t, 1 - odd).wait_send()
        rest_copy(t, 1 - odd).wait_send()

    @pl.when(carries)
    def _():
        for t in range(tiles):
            carry_copy(t).wait_send()

    for side in range(2):
        y_copy(side).wait_send()

    every_top().wait_send()
    every_top().wait_recv()
    peak = jnp.max(got[...], axis=0)
    next_speed[...] = jnp.broadcast_to(jnp.max(peak, axis=1, keepdims=True), next_speed.shape)


def finish(state, peak, new_state, next_speed, sem):
    comps = state.shape[0]
    copies = [
        pltpu.make_async_copy(state.at[c], new_state.at[c], sem.at[c]) for c in range(comps)
    ]
    copies.append(pltpu.make_async_copy(peak, next_speed, sem.at[comps]))
    for copy in copies:
        copy.start()
    for copy in copies:
        copy.wait()


def local(nx, ny, start_state, section_state, previous_speed):
    comps, cx, cy, nz = section_state.shape
    tiles = cy // ROWS
    f32 = jnp.float32
    dma = pltpu.SemaphoreType.DMA
    state, peak = pl.pallas_call(
        functools.partial(kernel, nx, ny),
        out_shape=(
            pltpu.VMEM(section_state.shape, f32),
            pltpu.VMEM((1, 128), f32),
        ),
        in_specs=[
            pl.BlockSpec(memory_space=pl.ANY),
            pl.BlockSpec(memory_space=pl.ANY),
            pl.BlockSpec(memory_space=pltpu.SMEM),
        ],
        out_specs=(
            pl.BlockSpec(memory_space=pltpu.VMEM),
            pl.BlockSpec(memory_space=pltpu.VMEM),
        ),
        scratch_shapes=[
            pltpu.VMEM(section_state.shape, f32),
            pltpu.VMEM(section_state.shape, f32),
            pltpu.VMEM(section_state.shape, f32),
            pltpu.VMEM((comps, cx + 2 * WIDTH, cy, nz), f32),
            pltpu.VMEM((comps, cx, cy + 2 * ROWS, nz), f32),
            pltpu.VMEM((comps - 1, cx + 2 * WIDTH, cy + 2 * ROWS, nz), f32),
            pltpu.VMEM((2, tiles, comps, WIDTH, ROWS, nz), f32),
            pltpu.VMEM((tiles, DETOUR, WIDTH, ROWS, nz), f32),
            pltpu.VMEM((comps, cx, ROWS, nz), f32),
            pltpu.VMEM((comps, cx, ROWS, nz), f32),
            pltpu.VMEM((1, 128), f32),
            pltpu.VMEM((nx * ny, 1, 128), f32),
            dma((2,)),
            dma((tiles,)),
            dma((tiles,)),
            dma((tiles,)),
            dma((tiles,)),
            dma((tiles,)),
            dma((tiles,)),
            dma((tiles,)),
            dma((tiles,)),
            dma((2,)),
            dma((2,)),
            dma,
            dma,
            pltpu.SemaphoreType.REGULAR((len(meeting_rounds(nx, ny)),)),
            pltpu.SemaphoreType.REGULAR,
        ],
        compiler_params=pltpu.CompilerParams(collective_id=0, has_side_effects=True),
        name="section_step",
    )(start_state, section_state, previous_speed.reshape(1, 1))
    new_state, next_speed = pl.pallas_call(
        finish,
        out_shape=(
            jax.ShapeDtypeStruct(section_state.shape, f32),
            jax.ShapeDtypeStruct((1, 128), f32),
        ),
        in_specs=[pl.BlockSpec(memory_space=pltpu.VMEM)] * 2,
        out_specs=(pl.BlockSpec(memory_space=pl.ANY), pl.BlockSpec(memory_space=pl.ANY)),
        scratch_shapes=[dma((comps + 1,))],
        name="write_out",
    )(
        pltpu.with_memory_space_constraint(state, pltpu.VMEM),
        pltpu.with_memory_space_constraint(peak, pltpu.VMEM),
    )
    return new_state, next_speed[0, 0]


def solution(mesh):
    nx, ny = mesh.shape["gx"], mesh.shape["gy"]
    in_specs = (P(None, "gx", "gy", None), P(None, "gx", "gy", None), P())
    out_specs = (P(None, "gx", "gy", None), P())
    return jax.shard_map(
        functools.partial(local, nx, ny),
        mesh=mesh,
        in_specs=in_specs,
        out_specs=out_specs,
        check_vma=False,
    )
```

```python
import functools

import jax
import jax.numpy as jnp
from jax import lax
from jax.experimental import pallas as pl
from jax.experimental.pallas import tpu as pltpu
from jax.sharding import PartitionSpec as P

GAMMA = 1.4
COURANT = 0.3
VISCOSITY = 0.05
CONDUCTION = 0.07
FIRST = (0.8, -0.2, 4.0 / 105.0, -1.0 / 280.0)
SECOND = (1.6, -0.2, 8.0 / 315.0, -1.0 / 560.0)
CENTRE = -205.0 / 72.0
WIDTH = 4
ROWS = 8
DETOUR = 1
MESH = pl.DeviceIdType.MESH


def primitive(q):
    density, m1, m2, m3, energy = q
    inverse = 1.0 / density
    u, v, w = m1 * inverse, m2 * inverse, m3 * inverse
    kinetic = 0.5 * (u * u + v * v + w * w)
    pressure = (GAMMA - 1.0) * (energy - density * kinetic)
    return inverse, (u, v, w), kinetic, pressure


def wave_speed(q):
    inverse, _, kinetic, pressure = primitive(q)
    return jnp.sqrt(2.0 * kinetic) + jnp.sqrt(GAMMA * (pressure * inverse))


def smooth_terms(primitives):
    inverse, (u, v, w), kinetic, pressure = primitives
    return [
        VISCOSITY * u,
        VISCOSITY * v,
        VISCOSITY * w,
        VISCOSITY * kinetic + CONDUCTION * (pressure * inverse),
    ]


def flux_terms(q, primitives, direction):
    _, velocity, _, pressure = primitives
    speed = velocity[direction]
    flux = [q[1 + direction]]
    for k in range(3):
        term = q[1 + k] * speed
        flux.append(term + pressure if k == direction else term)
    flux.append((q[4] + pressure) * speed)
    return flux


def meeting_rounds(nx, ny):
    rounds, known = [], 1
    while 2 * known < nx:
        rounds.append(("gx", known))
        known *= 2
    known = 0
    while 2 * known < ny:
        rounds.append(("gy", max(known, 1)))
        known = 2 * known if known else 1
    return rounds


def kernel(
    nx, ny, start, section, speed, out, next_speed,
    old, sec, acc, fx, fy, sm, xhalo, relay, ylo, yhi, top, got,
    load_sem, ns_sem, nr_sem, fs_sem, fr_sem, ds_sem, dr_sem, rr_sem, rs_sem,
    ys_sem, yr_sem, ts_sem, tr_sem, meet_sem, ring_sem,
):
    _, cx, cy, nz = old.shape
    tiles = cy // ROWS
    devices = nx * ny
    me_x, me_y = lax.axis_index("gx"), lax.axis_index("gy")
    odd = lax.rem(me_x, 2)

    def on_x(k):
        return (lax.rem(me_x + k, nx), me_y)

    def on_y(k):
        return (me_x, lax.rem(me_y + k, ny))

    first, last = me_x == 0, me_x == nx - 1
    near, far = on_x(nx + 1 - 2 * odd), on_x(nx - 1 + 2 * odd)
    beyond = on_x(nx + 2 - 4 * odd)
    detours = first | ((odd == 1) & (me_x < nx - 1))
    carries = (me_x == 1) | ((odd == 0) & (me_x < nx - 2))

    barrier = pltpu.get_barrier_semaphore()

    def greet(device, sem=barrier):
        pl.semaphore_signal(sem, inc=1, device_id=device, device_id_type=MESH)

    for device in (near, on_y(1), on_y(ny - 1)):
        greet(device)

    @pl.when((odd == 0) & (me_x > 0))
    def _():
        greet(far)

    load_section = pltpu.make_async_copy(section, sec, load_sem.at[0])
    load_start = pltpu.make_async_copy(start, old, load_sem.at[1])
    load_start.start()
    load_section.start()

    direct = old.shape[0] - DETOUR

    def remote(src, dst, send_sem, recv_sem, device):
        return pltpu.make_async_remote_copy(
            src_ref=src,
            dst_ref=dst,
            send_sem=send_sem,
            recv_sem=recv_sem,
            device_id=device,
            device_id_type=MESH,
        )

    slabs = [(t, 0, WIDTH) for t in range(tiles - 1)]
    slabs += [(tiles - 1, 1, WIDTH - 1), (tiles - 1, 0, 1)]

    def layers_of(side, h, count):
        return pl.ds(h + side * (WIDTH - 2 * h - count), count)

    def edge_of(side, t, comps, h=0, count=WIDTH):
        layers = layers_of(side, h, count)
        layers = pl.ds((1 - side) * (cx - WIDTH) + layers.start, count)
        return old.at[comps, layers, pl.ds(t * ROWS, ROWS), :]

    def near_copy(n, side):
        t, h, count = slabs[n]
        every = pl.ds(0, old.shape[0])
        return remote(
            edge_of(odd, t, every, h, count),
            xhalo.at[side, t, every, layers_of(side, h, count)],
            ns_sem.at[n], nr_sem.at[n], near,
        )

    def far_copy(n, side):
        t, h, count = slabs[n]
        some = pl.ds(0, direct)
        return remote(
            edge_of(1 - odd, t, some, h, count),
            xhalo.at[side, t, some, layers_of(side, h, count)],
            fs_sem.at[n], fr_sem.at[n], far,
        )

    def rest_copy(t, side):
        rest = pl.ds(direct, DETOUR)
        return remote(
            edge_of(1 - odd, t, rest), xhalo.at[side, t, rest], ds_sem.at[t], dr_sem.at[t], far
        )

    def detour_copy(t):
        rest = pl.ds(direct, DETOUR)
        return remote(edge_of(1 - odd, t, rest), relay.at[t], ds_sem.at[t], rr_sem.at[t], near)

    def carry_copy(t):
        rest = pl.ds(direct, DETOUR)
        return remote(
            relay.at[t], xhalo.at[odd, t, rest], rs_sem.at[t], dr_sem.at[t], beyond
        )

    def y_copy(side):
        rows = pl.ds(cy - ROWS, ROWS) if side == 0 else pl.ds(0, ROWS)
        return pltpu.make_async_remote_copy(
            src_ref=old.at[:, :, rows, :],
            dst_ref=ylo if side == 0 else yhi,
            send_sem=ys_sem.at[side],
            recv_sem=yr_sem.at[side],
            device_id=on_y(1) if side == 0 else on_y(ny - 1),
            device_id_type=MESH,
        )

    def start_far():
        for n in range(len(slabs)):
            far_copy(n, 1 - odd).start()

        @pl.when(jnp.logical_not(detours))
        def _():
            for t in range(tiles):
                rest_copy(t, 1 - odd).start()

    load_start.wait()
    pl.semaphore_wait(barrier, jnp.where(odd == 1, 4, 3))

    @pl.when(first)
    def _():
        greet(far)

    @pl.when(odd == 1)
    def _():
        greet(far, ring_sem)

    @pl.when(last)
    def _():
        greet(on_x(2), ring_sem)

    @pl.when(detours)
    def _():
        for t in range(tiles):
            detour_copy(t).start()

    @pl.when(odd == 1)
    def _():
        start_far()

    for n in range(len(slabs)):
        near_copy(n, odd).start()
    for side in range(2):
        y_copy(side).start()

    @pl.when((odd == 0) & (me_x > 0))
    def _():
        pl.semaphore_wait(ring_sem, 1)
        start_far()

    rounds = meeting_rounds(nx, ny)

    def meet(r):
        axis, distance = rounds[r]
        for k in (distance, -distance):
            device = on_x(nx + k) if axis == "gx" else on_y(ny + k)
            pl.semaphore_signal(meet_sem.at[r], inc=1, device_id=device, device_id_type=MESH)

    def met(r):
        pl.semaphore_wait(meet_sem.at[r], 2)
        if r + 1 < len(rounds):
            meet(r + 1)

    scale = 0.25 * (COURANT / speed[0, 0])

    edge = jnp.zeros((WIDTH, cy, nz), jnp.float32)
    for c in range(5):
        fx[c, 0:WIDTH] = edge
        fx[c, cx + WIDTH : cx + 2 * WIDTH] = edge
    for c in range(4):
        sm[c, 0:WIDTH, ROWS : ROWS + cy] = edge
        sm[c, cx + WIDTH : cx + 2 * WIDTH, ROWS : ROWS + cy] = edge

    load_section.wait()

    def along_z(i, _):
        q = [sec[c, i] for c in range(5)]
        prim = primitive(q)
        smooth = smooth_terms(prim)
        for c, term in enumerate(flux_terms(q, prim, 0)):
            fx[c, i + WIDTH] = term
        for c, term in enumerate(flux_terms(q, prim, 1)):
            fy[c, i, ROWS : ROWS + cy] = term
        for c, term in enumerate(smooth):
            sm[c, i + WIDTH, ROWS : ROWS + cy] = term
        for c, term in enumerate(flux_terms(q, prim, 2)):
            total = None
            for m in range(1, WIDTH + 1):
                f = FIRST[m - 1] * term
                if c > 0:
                    s = SECOND[m - 1] * smooth[c - 1]
                    above, below = s - f, s + f
                else:
                    above, below = -f, f
                pair = pltpu.roll(above, nz - m, 1) + pltpu.roll(below, m, 1)
                total = pair if total is None else total + pair
            if c > 0:
                total = total + (3.0 * CENTRE) * smooth[c - 1]
            acc[c, i] = total
        return 0

    lax.fori_loop(0, cx, along_z, 0)

    @pl.when(first | (me_x == 1))
    def _():
        pl.semaphore_wait(ring_sem, 1)

    @pl.when(first)
    def _():
        start_far()

    @pl.when(carries)
    def _():
        for t in range(tiles):
            detour_copy(t).wait_recv()
            carry_copy(t).start()

    meet(0)

    def along_x(i, _):
        for c in range(5):
            total = acc[c, i]
            for m in range(1, WIDTH + 1):
                total = total - FIRST[m - 1] * (fx[c, i + WIDTH + m] - fx[c, i + WIDTH - m])
                if c > 0:
                    total = total + SECOND[m - 1] * (
                        sm[c - 1, i + WIDTH + m, ROWS : ROWS + cy]
                        + sm[c - 1, i + WIDTH - m, ROWS : ROWS + cy]
                    )
            acc[c, i] = total
        return 0

    lax.fori_loop(0, cx, along_x, 0)
    met(0)
    met(1)

    y_copy(0).wait_recv()
    y_copy(1).wait_recv()

    def along_y(i, _):
        for halo, first in ((ylo, 0), (yhi, ROWS + cy)):
            q = [halo[c, i] for c in range(5)]
            prim = primitive(q)
            for c, term in enumerate(flux_terms(q, prim, 1)):
                fy[c, i, first : first + ROWS] = term
            for c, term in enumerate(smooth_terms(prim)):
                sm[c, i + WIDTH, first : first + ROWS] = term
        for c in range(5):
            total = acc[c, i]
            for m in range(1, WIDTH + 1):
                above, below = ROWS + m, ROWS - m
                total = total - FIRST[m - 1] * (
                    fy[c, i, above : above + cy] - fy[c, i, below : below + cy]
                )
                if c > 0:
                    total = total + SECOND[m - 1] * (
                        sm[c - 1, i + WIDTH, above : above + cy]
                        + sm[c - 1, i + WIDTH, below : below + cy]
                    )
            acc[c, i] = total
        return 0

    lax.fori_loop(0, cx, along_y, 0)
    met(2)
    for r in range(3, len(rounds)):
        met(r)

    largest = None
    for n, (t, first_h, count) in enumerate(slabs):
        ends = n + 1 == len(slabs) or slabs[n + 1][0] != t
        rows = slice(t * ROWS, (t + 1) * ROWS)
        for turn in range(2):
            if turn == 0:
                side = odd
                far_copy(n, side).wait_recv()
                if first_h + count == WIDTH:
                    rest_copy(t, side).wait_recv()
            else:
                side = 1 - odd
                near_copy(n, side).wait_recv()
            sign = (1 - 2 * side).astype(jnp.float32)
            inner = [side * (cx - 1 - 2 * i) + i for i in range(WIDTH)]
            touched = range(first_h + count)
            totals = [[acc[c, inner[i], rows] for c in range(5)] for i in touched]
            for h in range(first_h, first_h + count):
                q = [xhalo[side, t, c, side * (WIDTH - 1 - 2 * h) + h] for c in range(5)]
                prim = primitive(q)
                flux = [sign * f for f in flux_terms(q, prim, 0)]
                smooth = smooth_terms(prim)
                for i in range(h + 1):
                    m = i + WIDTH - h
                    for c in range(5):
                        term = FIRST[m - 1] * flux[c]
                        if c > 0:
                            term = term + SECOND[m - 1] * smooth[c - 1]
                        totals[i][c] = totals[i][c] + term
            for i in touched:
                if not ends and i < first_h:
                    for c in range(5):
                        acc[c, inner[i], rows] = totals[i][c]
                    continue
                new = []
                for c in range(5):
                    value = (
                        0.75 * old[c, inner[i], rows]
                        + 0.25 * sec[c, inner[i], rows]
                        + scale * totals[i][c]
                    )
                    out[c, inner[i], rows] = value
                    new.append(value)
                wave = wave_speed(new)
                largest = wave if largest is None else jnp.maximum(largest, wave)

    me = me_x * ny + me_y

    def top_copy(k):
        to = k + (k >= me).astype(jnp.int32)
        return remote(top, got.at[me], ts_sem, tr_sem, (to // ny, lax.rem(to, ny)))

    def every_top():
        others = pl.ds(0, devices - 1)
        return remote(got.at[others], got.at[others], ts_sem, tr_sem, near)

    folded = largest[:, 0:128]
    for first in range(128, nz, 128):
        folded = jnp.maximum(folded, largest[:, first : first + 128])
    peak = jnp.max(folded, axis=0, keepdims=True)
    top[...] = peak

    def send(k, _):
        top_copy(k).start()
        return 0

    lax.fori_loop(0, devices - 1, send, 0, unroll=devices <= 64)
    got[me] = peak
    for n in range(len(slabs)):
        near_copy(n, odd).wait_send()
        far_copy(n, 1 - odd).wait_send()
    for t in range(tiles):
        rest_copy(t, 1 - odd).wait_send()

    @pl.when(carries)
    def _():
        for t in range(tiles):
            carry_copy(t).wait_send()

    for side in range(2):
        y_copy(side).wait_send()

    every_top().wait_send()
    every_top().wait_recv()
    peak = jnp.max(got[...], axis=0)
    next_speed[...] = jnp.broadcast_to(jnp.max(peak, axis=1, keepdims=True), next_speed.shape)


def finish(state, peak, new_state, next_speed, sem):
    comps = state.shape[0]
    copies = [
        pltpu.make_async_copy(state.at[c], new_state.at[c], sem.at[c]) for c in range(comps)
    ]
    copies.append(pltpu.make_async_copy(peak, next_speed, sem.at[comps]))
    for copy in copies:
        copy.start()
    for copy in copies:
        copy.wait()


def local(nx, ny, start_state, section_state, previous_speed):
    comps, cx, cy, nz = section_state.shape
    tiles = cy // ROWS
    f32 = jnp.float32
    dma = pltpu.SemaphoreType.DMA
    state, peak = pl.pallas_call(
        functools.partial(kernel, nx, ny),
        out_shape=(
            pltpu.VMEM(section_state.shape, f32),
            pltpu.VMEM((1, 128), f32),
        ),
        in_specs=[
            pl.BlockSpec(memory_space=pl.ANY),
            pl.BlockSpec(memory_space=pl.ANY),
            pl.BlockSpec(memory_space=pltpu.SMEM),
        ],
        out_specs=(
            pl.BlockSpec(memory_space=pltpu.VMEM),
            pl.BlockSpec(memory_space=pltpu.VMEM),
        ),
        scratch_shapes=[
            pltpu.VMEM(section_state.shape, f32),
            pltpu.VMEM(section_state.shape, f32),
            pltpu.VMEM(section_state.shape, f32),
            pltpu.VMEM((comps, cx + 2 * WIDTH, cy, nz), f32),
            pltpu.VMEM((comps, cx, cy + 2 * ROWS, nz), f32),
            pltpu.VMEM((comps - 1, cx + 2 * WIDTH, cy + 2 * ROWS, nz), f32),
            pltpu.VMEM((2, tiles, comps, WIDTH, ROWS, nz), f32),
            pltpu.VMEM((tiles, DETOUR, WIDTH, ROWS, nz), f32),
            pltpu.VMEM((comps, cx, ROWS, nz), f32),
            pltpu.VMEM((comps, cx, ROWS, nz), f32),
            pltpu.VMEM((1, 128), f32),
            pltpu.VMEM((nx * ny, 1, 128), f32),
            dma((2,)),
            dma((tiles + 1,)),
            dma((tiles + 1,)),
            dma((tiles + 1,)),
            dma((tiles + 1,)),
            dma((tiles,)),
            dma((tiles,)),
            dma((tiles,)),
            dma((tiles,)),
            dma((2,)),
            dma((2,)),
            dma,
            dma,
            pltpu.SemaphoreType.REGULAR((len(meeting_rounds(nx, ny)),)),
            pltpu.SemaphoreType.REGULAR,
        ],
        compiler_params=pltpu.CompilerParams(collective_id=0, has_side_effects=True),
        name="section_step",
    )(start_state, section_state, previous_speed.reshape(1, 1))
    new_state, next_speed = pl.pallas_call(
        finish,
        out_shape=(
            jax.ShapeDtypeStruct(section_state.shape, f32),
            jax.ShapeDtypeStruct((1, 128), f32),
        ),
        in_specs=[pl.BlockSpec(memory_space=pltpu.VMEM)] * 2,
        out_specs=(pl.BlockSpec(memory_space=pl.ANY), pl.BlockSpec(memory_space=pl.ANY)),
        scratch_shapes=[dma((comps + 1,))],
        name="write_out",
    )(
        pltpu.with_memory_space_constraint(state, pltpu.VMEM),
        pltpu.with_memory_space_constraint(peak, pltpu.VMEM),
    )
    return new_state, next_speed[0, 0]


def solution(mesh):
    nx, ny = mesh.shape["gx"], mesh.shape["gy"]
    in_specs = (P(None, "gx", "gy", None), P(None, "gx", "gy", None), P())
    out_specs = (P(None, "gx", "gy", None), P())
    return jax.shard_map(
        functools.partial(local, nx, ny),
        mesh=mesh,
        in_specs=in_specs,
        out_specs=out_specs,
        check_vma=False,
    )
```

```python
import functools

import jax
import jax.numpy as jnp
from jax import lax
from jax.experimental import pallas as pl
from jax.experimental.pallas import tpu as pltpu
from jax.sharding import PartitionSpec as P

GAMMA = 1.4
COURANT = 0.3
VISCOSITY = 0.05
CONDUCTION = 0.07
FIRST = (0.8, -0.2, 4.0 / 105.0, -1.0 / 280.0)
SECOND = (1.6, -0.2, 8.0 / 315.0, -1.0 / 560.0)
CENTRE = -205.0 / 72.0
WIDTH = 4
ROWS = 8
DETOUR = 1
MESH = pl.DeviceIdType.MESH


def primitive(q):
    density, m1, m2, m3, energy = q
    inverse = 1.0 / density
    u, v, w = m1 * inverse, m2 * inverse, m3 * inverse
    kinetic = 0.5 * (u * u + v * v + w * w)
    pressure = (GAMMA - 1.0) * (energy - density * kinetic)
    return inverse, (u, v, w), kinetic, pressure


def wave_speed(q):
    inverse, _, kinetic, pressure = primitive(q)
    return jnp.sqrt(2.0 * kinetic) + jnp.sqrt(GAMMA * (pressure * inverse))


def smooth_terms(primitives):
    inverse, (u, v, w), kinetic, pressure = primitives
    return [
        VISCOSITY * u,
        VISCOSITY * v,
        VISCOSITY * w,
        VISCOSITY * kinetic + CONDUCTION * (pressure * inverse),
    ]


def flux_terms(q, primitives, direction):
    _, velocity, _, pressure = primitives
    speed = velocity[direction]
    flux = [q[1 + direction]]
    for k in range(3):
        term = q[1 + k] * speed
        flux.append(term + pressure if k == direction else term)
    flux.append((q[4] + pressure) * speed)
    return flux


def meeting_rounds(nx, ny):
    rounds, known = [], 1
    while 2 * known < nx:
        rounds.append(("gx", known))
        known *= 2
    known = 0
    while 2 * known < ny:
        rounds.append(("gy", max(known, 1)))
        known = 2 * known if known else 1
    return rounds


def kernel(
    nx, ny, start, section, speed, out, next_speed,
    old, sec, acc, fx, fy, sm, xhalo, relay, ylo, yhi, top, got,
    load_sem, ns_sem, nr_sem, fs_sem, fr_sem, ds_sem, dr_sem, rr_sem, rs_sem,
    ys_sem, yr_sem, ts_sem, tr_sem, meet_sem, ring_sem,
):
    _, cx, cy, nz = old.shape
    tiles = cy // ROWS
    devices = nx * ny
    me_x, me_y = lax.axis_index("gx"), lax.axis_index("gy")
    odd = lax.rem(me_x, 2)

    def on_x(k):
        return (lax.rem(me_x + k, nx), me_y)

    def on_y(k):
        return (me_x, lax.rem(me_y + k, ny))

    first, last = me_x == 0, me_x == nx - 1
    near, far = on_x(nx + 1 - 2 * odd), on_x(nx - 1 + 2 * odd)
    beyond = on_x(nx + 2 - 4 * odd)
    detours = first | ((odd == 1) & (me_x < nx - 1))
    carries = (me_x == 1) | ((odd == 0) & (me_x < nx - 2))

    barrier = pltpu.get_barrier_semaphore()

    def greet(device, sem=barrier):
        pl.semaphore_signal(sem, inc=1, device_id=device, device_id_type=MESH)

    for device in (near, on_y(1), on_y(ny - 1)):
        greet(device)

    @pl.when((odd == 0) & (me_x > 0))
    def _():
        greet(far)

    load_section = pltpu.make_async_copy(section, sec, load_sem.at[0])
    load_start = pltpu.make_async_copy(start, old, load_sem.at[1])
    load_start.start()
    load_section.start()

    direct = old.shape[0] - DETOUR

    def remote(src, dst, send_sem, recv_sem, device):
        return pltpu.make_async_remote_copy(
            src_ref=src,
            dst_ref=dst,
            send_sem=send_sem,
            recv_sem=recv_sem,
            device_id=device,
            device_id_type=MESH,
        )

    slabs = [(t, 0, WIDTH) for t in range(tiles - 1)]
    slabs += [(tiles - 1, 1, WIDTH - 1), (tiles - 1, 0, 1)]

    def layers_of(side, h, count):
        return pl.ds(h + side * (WIDTH - 2 * h - count), count)

    def edge_of(side, t, comps, h=0, count=WIDTH):
        layers = layers_of(side, h, count)
        layers = pl.ds((1 - side) * (cx - WIDTH) + layers.start, count)
        return old.at[comps, layers, pl.ds(t * ROWS, ROWS), :]

    def near_copy(n, side):
        t, h, count = slabs[n]
        every = pl.ds(0, old.shape[0])
        return remote(
            edge_of(odd, t, every, h, count),
            xhalo.at[side, t, every, layers_of(side, h, count)],
            ns_sem.at[n], nr_sem.at[n], near,
        )

    def far_copy(n, side):
        t, h, count = slabs[n]
        some = pl.ds(0, direct)
        return remote(
            edge_of(1 - odd, t, some, h, count),
            xhalo.at[side, t, some, layers_of(side, h, count)],
            fs_sem.at[n], fr_sem.at[n], far,
        )

    def rest_copy(t, side):
        rest = pl.ds(direct, DETOUR)
        return remote(
            edge_of(1 - odd, t, rest), xhalo.at[side, t, rest], ds_sem.at[t], dr_sem.at[t], far
        )

    def detour_copy(t):
        rest = pl.ds(direct, DETOUR)
        return remote(edge_of(1 - odd, t, rest), relay.at[t], ds_sem.at[t], rr_sem.at[t], near)

    def carry_copy(t):
        rest = pl.ds(direct, DETOUR)
        return remote(
            relay.at[t], xhalo.at[odd, t, rest], rs_sem.at[t], dr_sem.at[t], beyond
        )

    def y_copy(side):
        rows = pl.ds(cy - ROWS, ROWS) if side == 0 else pl.ds(0, ROWS)
        return pltpu.make_async_remote_copy(
            src_ref=old.at[:, :, rows, :],
            dst_ref=ylo if side == 0 else yhi,
            send_sem=ys_sem.at[side],
            recv_sem=yr_sem.at[side],
            device_id=on_y(1) if side == 0 else on_y(ny - 1),
            device_id_type=MESH,
        )

    def start_far():
        for n in range(len(slabs)):
            far_copy(n, 1 - odd).start()

        @pl.when(jnp.logical_not(detours))
        def _():
            for t in range(tiles):
                rest_copy(t, 1 - odd).start()

    load_start.wait()
    pl.semaphore_wait(barrier, jnp.where(odd == 1, 4, 3))

    @pl.when(first)
    def _():
        greet(far)

    @pl.when(odd == 1)
    def _():
        greet(far, ring_sem)

    @pl.when(last)
    def _():
        greet(on_x(2), ring_sem)

    @pl.when(detours)
    def _():
        for t in range(tiles):
            detour_copy(t).start()

    @pl.when(odd == 1)
    def _():
        start_far()

    for n in range(len(slabs)):
        near_copy(n, odd).start()
    @pl.when((odd == 0) & (me_x > 0))
    def _():
        pl.semaphore_wait(ring_sem, 1)
        start_far()

    for side in range(2):
        y_copy(side).start()

    rounds = meeting_rounds(nx, ny)

    def meet(r):
        axis, distance = rounds[r]
        for k in (distance, -distance):
            device = on_x(nx + k) if axis == "gx" else on_y(ny + k)
            pl.semaphore_signal(meet_sem.at[r], inc=1, device_id=device, device_id_type=MESH)

    def met(r):
        pl.semaphore_wait(meet_sem.at[r], 2)
        if r + 1 < len(rounds):
            meet(r + 1)

    scale = 0.25 * (COURANT / speed[0, 0])

    edge = jnp.zeros((WIDTH, cy, nz), jnp.float32)
    for c in range(5):
        fx[c, 0:WIDTH] = edge
        fx[c, cx + WIDTH : cx + 2 * WIDTH] = edge
    for c in range(4):
        sm[c, 0:WIDTH, ROWS : ROWS + cy] = edge
        sm[c, cx + WIDTH : cx + 2 * WIDTH, ROWS : ROWS + cy] = edge

    load_section.wait()

    def along_z(i, _):
        q = [sec[c, i] for c in range(5)]
        prim = primitive(q)
        smooth = smooth_terms(prim)
        for c, term in enumerate(flux_terms(q, prim, 0)):
            fx[c, i + WIDTH] = term
        for c, term in enumerate(flux_terms(q, prim, 1)):
            fy[c, i, ROWS : ROWS + cy] = term
        for c, term in enumerate(smooth):
            sm[c, i + WIDTH, ROWS : ROWS + cy] = term
        for c, term in enumerate(flux_terms(q, prim, 2)):
            total = None
            for m in range(1, WIDTH + 1):
                f = FIRST[m - 1] * term
                if c > 0:
                    s = SECOND[m - 1] * smooth[c - 1]
                    above, below = s - f, s + f
                else:
                    above, below = -f, f
                pair = pltpu.roll(above, nz - m, 1) + pltpu.roll(below, m, 1)
                total = pair if total is None else total + pair
            if c > 0:
                total = total + (3.0 * CENTRE) * smooth[c - 1]
            acc[c, i] = total
        return 0

    lax.fori_loop(0, cx, along_z, 0)

    @pl.when(first | (me_x == 1))
    def _():
        pl.semaphore_wait(ring_sem, 1)

    @pl.when(first)
    def _():
        start_far()

    @pl.when(carries)
    def _():
        for t in range(tiles):
            detour_copy(t).wait_recv()
            carry_copy(t).start()

    meet(0)

    def along_x(i, _):
        for c in range(5):
            total = acc[c, i]
            for m in range(1, WIDTH + 1):
                total = total - FIRST[m - 1] * (fx[c, i + WIDTH + m] - fx[c, i + WIDTH - m])
                if c > 0:
                    total = total + SECOND[m - 1] * (
                        sm[c - 1, i + WIDTH + m, ROWS : ROWS + cy]
                        + sm[c - 1, i + WIDTH - m, ROWS : ROWS + cy]
                    )
            acc[c, i] = total
        return 0

    lax.fori_loop(0, cx, along_x, 0)
    met(0)
    met(1)

    y_copy(0).wait_recv()
    y_copy(1).wait_recv()

    def along_y(i, _):
        for halo, first in ((ylo, 0), (yhi, ROWS + cy)):
            q = [halo[c, i] for c in range(5)]
            prim = primitive(q)
            for c, term in enumerate(flux_terms(q, prim, 1)):
                fy[c, i, first : first + ROWS] = term
            for c, term in enumerate(smooth_terms(prim)):
                sm[c, i + WIDTH, first : first + ROWS] = term
        for c in range(5):
            total = acc[c, i]
            for m in range(1, WIDTH + 1):
                above, below = ROWS + m, ROWS - m
                total = total - FIRST[m - 1] * (
                    fy[c, i, above : above + cy] - fy[c, i, below : below + cy]
                )
                if c > 0:
                    total = total + SECOND[m - 1] * (
                        sm[c - 1, i + WIDTH, above : above + cy]
                        + sm[c - 1, i + WIDTH, below : below + cy]
                    )
            acc[c, i] = total
        return 0

    lax.fori_loop(0, cx, along_y, 0)
    met(2)
    for r in range(3, len(rounds)):
        met(r)

    largest = None
    for n, (t, first_h, count) in enumerate(slabs):
        ends = n + 1 == len(slabs) or slabs[n + 1][0] != t
        rows = slice(t * ROWS, (t + 1) * ROWS)
        if count == 1:
            far_copy(n, odd).wait_recv()
            near_copy(n, 1 - odd).wait_recv()
        for turn in range(2):
            if turn == 0:
                side = odd
                if count > 1:
                    far_copy(n, side).wait_recv()
                if first_h + count == WIDTH:
                    rest_copy(t, side).wait_recv()
            else:
                side = 1 - odd
                if count > 1:
                    near_copy(n, side).wait_recv()
            sign = (1 - 2 * side).astype(jnp.float32)
            inner = [side * (cx - 1 - 2 * i) + i for i in range(WIDTH)]
            touched = range(first_h + count)
            totals = [[acc[c, inner[i], rows] for c in range(5)] for i in touched]
            for h in range(first_h, first_h + count):
                q = [xhalo[side, t, c, side * (WIDTH - 1 - 2 * h) + h] for c in range(5)]
                prim = primitive(q)
                flux = [sign * f for f in flux_terms(q, prim, 0)]
                smooth = smooth_terms(prim)
                for i in range(h + 1):
                    m = i + WIDTH - h
                    for c in range(5):
                        term = FIRST[m - 1] * flux[c]
                        if c > 0:
                            term = term + SECOND[m - 1] * smooth[c - 1]
                        totals[i][c] = totals[i][c] + term
            for i in touched:
                if not ends and i < first_h:
                    for c in range(5):
                        acc[c, inner[i], rows] = totals[i][c]
                    continue
                new = []
                for c in range(5):
                    value = (
                        0.75 * old[c, inner[i], rows]
                        + 0.25 * sec[c, inner[i], rows]
                        + scale * totals[i][c]
                    )
                    out[c, inner[i], rows] = value
                    new.append(value)
                wave = wave_speed(new)
                largest = wave if largest is None else jnp.maximum(largest, wave)

    me = me_x * ny + me_y

    def top_copy(k):
        to = k + (k >= me).astype(jnp.int32)
        return remote(top, got.at[me], ts_sem, tr_sem, (to // ny, lax.rem(to, ny)))

    def every_top():
        others = pl.ds(0, devices - 1)
        return remote(got.at[others], got.at[others], ts_sem, tr_sem, near)

    folded = largest[:, 0:128]
    for first in range(128, nz, 128):
        folded = jnp.maximum(folded, largest[:, first : first + 128])
    peak = jnp.max(folded, axis=0, keepdims=True)
    top[...] = peak

    def send(k, _):
        top_copy(k).start()
        return 0

    lax.fori_loop(0, devices - 1, send, 0, unroll=devices <= 64)
    got[me] = peak
    for n in range(len(slabs)):
        near_copy(n, odd).wait_send()
        far_copy(n, 1 - odd).wait_send()
    for t in range(tiles):
        rest_copy(t, 1 - odd).wait_send()

    @pl.when(carries)
    def _():
        for t in range(tiles):
            carry_copy(t).wait_send()

    for side in range(2):
        y_copy(side).wait_send()

    every_top().wait_send()
    every_top().wait_recv()
    peak = jnp.max(got[...], axis=0)
    next_speed[...] = jnp.broadcast_to(jnp.max(peak, axis=1, keepdims=True), next_speed.shape)


def finish(state, peak, new_state, next_speed, sem):
    comps = state.shape[0]
    copies = [
        pltpu.make_async_copy(state.at[c], new_state.at[c], sem.at[c]) for c in range(comps)
    ]
    copies.append(pltpu.make_async_copy(peak, next_speed, sem.at[comps]))
    for copy in copies:
        copy.start()
    for copy in copies:
        copy.wait()


def local(nx, ny, start_state, section_state, previous_speed):
    comps, cx, cy, nz = section_state.shape
    tiles = cy // ROWS
    f32 = jnp.float32
    dma = pltpu.SemaphoreType.DMA
    state, peak = pl.pallas_call(
        functools.partial(kernel, nx, ny),
        out_shape=(
            pltpu.VMEM(section_state.shape, f32),
            pltpu.VMEM((1, 128), f32),
        ),
        in_specs=[
            pl.BlockSpec(memory_space=pl.ANY),
            pl.BlockSpec(memory_space=pl.ANY),
            pl.BlockSpec(memory_space=pltpu.SMEM),
        ],
        out_specs=(
            pl.BlockSpec(memory_space=pltpu.VMEM),
            pl.BlockSpec(memory_space=pltpu.VMEM),
        ),
        scratch_shapes=[
            pltpu.VMEM(section_state.shape, f32),
            pltpu.VMEM(section_state.shape, f32),
            pltpu.VMEM(section_state.shape, f32),
            pltpu.VMEM((comps, cx + 2 * WIDTH, cy, nz), f32),
            pltpu.VMEM((comps, cx, cy + 2 * ROWS, nz), f32),
            pltpu.VMEM((comps - 1, cx + 2 * WIDTH, cy + 2 * ROWS, nz), f32),
            pltpu.VMEM((2, tiles, comps, WIDTH, ROWS, nz), f32),
            pltpu.VMEM((tiles, DETOUR, WIDTH, ROWS, nz), f32),
            pltpu.VMEM((comps, cx, ROWS, nz), f32),
            pltpu.VMEM((comps, cx, ROWS, nz), f32),
            pltpu.VMEM((1, 128), f32),
            pltpu.VMEM((nx * ny, 1, 128), f32),
            dma((2,)),
            dma((tiles + 1,)),
            dma((tiles + 1,)),
            dma((tiles + 1,)),
            dma((tiles + 1,)),
            dma((tiles,)),
            dma((tiles,)),
            dma((tiles,)),
            dma((tiles,)),
            dma((2,)),
            dma((2,)),
            dma,
            dma,
            pltpu.SemaphoreType.REGULAR((len(meeting_rounds(nx, ny)),)),
            pltpu.SemaphoreType.REGULAR,
        ],
        compiler_params=pltpu.CompilerParams(collective_id=0, has_side_effects=True),
        name="section_step",
    )(start_state, section_state, previous_speed.reshape(1, 1))
    new_state, next_speed = pl.pallas_call(
        finish,
        out_shape=(
            jax.ShapeDtypeStruct(section_state.shape, f32),
            jax.ShapeDtypeStruct((1, 128), f32),
        ),
        in_specs=[pl.BlockSpec(memory_space=pltpu.VMEM)] * 2,
        out_specs=(pl.BlockSpec(memory_space=pl.ANY), pl.BlockSpec(memory_space=pl.ANY)),
        scratch_shapes=[dma((comps + 1,))],
        name="write_out",
    )(
        pltpu.with_memory_space_constraint(state, pltpu.VMEM),
        pltpu.with_memory_space_constraint(peak, pltpu.VMEM),
    )
    return new_state, next_speed[0, 0]


def solution(mesh):
    nx, ny = mesh.shape["gx"], mesh.shape["gy"]
    in_specs = (P(None, "gx", "gy", None), P(None, "gx", "gy", None), P())
    out_specs = (P(None, "gx", "gy", None), P())
    return jax.shard_map(
        functools.partial(local, nx, ny),
        mesh=mesh,
        in_specs=in_specs,
        out_specs=out_specs,
        check_vma=False,
    )
```

```python
import functools

import jax
import jax.numpy as jnp
from jax import lax
from jax.experimental import pallas as pl
from jax.experimental.pallas import tpu as pltpu
from jax.sharding import PartitionSpec as P

GAMMA = 1.4
COURANT = 0.3
VISCOSITY = 0.05
CONDUCTION = 0.07
FIRST = (0.8, -0.2, 4.0 / 105.0, -1.0 / 280.0)
SECOND = (1.6, -0.2, 8.0 / 315.0, -1.0 / 560.0)
CENTRE = -205.0 / 72.0
WIDTH = 4
ROWS = 8
DETOUR = 1
MESH = pl.DeviceIdType.MESH


def primitive(q):
    density, m1, m2, m3, energy = q
    inverse = 1.0 / density
    u, v, w = m1 * inverse, m2 * inverse, m3 * inverse
    kinetic = 0.5 * (u * u + v * v + w * w)
    pressure = (GAMMA - 1.0) * (energy - density * kinetic)
    return inverse, (u, v, w), kinetic, pressure


def wave_speed(q):
    inverse, _, kinetic, pressure = primitive(q)
    return jnp.sqrt(2.0 * kinetic) + jnp.sqrt(GAMMA * (pressure * inverse))


def smooth_terms(primitives):
    inverse, (u, v, w), kinetic, pressure = primitives
    return [
        VISCOSITY * u,
        VISCOSITY * v,
        VISCOSITY * w,
        VISCOSITY * kinetic + CONDUCTION * (pressure * inverse),
    ]


def flux_terms(q, primitives, direction):
    _, velocity, _, pressure = primitives
    speed = velocity[direction]
    flux = [q[1 + direction]]
    for k in range(3):
        term = q[1 + k] * speed
        flux.append(term + pressure if k == direction else term)
    flux.append((q[4] + pressure) * speed)
    return flux


def meeting_rounds(nx, ny):
    rounds, known = [], 1
    while 2 * known < nx:
        rounds.append(("gx", known))
        known *= 2
    known = 0
    while 2 * known < ny:
        rounds.append(("gy", max(known, 1)))
        known = 2 * known if known else 1
    return rounds


def kernel(
    nx, ny, start, section, speed, out, next_speed,
    old, sec, acc, fx, fy, sm, xhalo, relay, aside, ylo, yhi, top, got,
    load_sem, ns_sem, nr_sem, fs_sem, fr_sem, ds_sem, dr_sem, rr_sem, rs_sem, sides_sem, sider_sem,
    ys_sem, yr_sem, ts_sem, tr_sem, meet_sem, ring_sem,
):
    _, cx, cy, nz = old.shape
    tiles = cy // ROWS
    devices = nx * ny
    me_x, me_y = lax.axis_index("gx"), lax.axis_index("gy")
    odd = lax.rem(me_x, 2)

    def on_x(k):
        return (lax.rem(me_x + k, nx), me_y)

    def on_y(k):
        return (me_x, lax.rem(me_y + k, ny))

    first, last = me_x == 0, me_x == nx - 1
    near, far = on_x(nx + 1 - 2 * odd), on_x(nx - 1 + 2 * odd)
    beyond = on_x(nx + 2 - 4 * odd)
    sidesteps, steps = me_x == nx // 2, me_x == nx // 2 - 1
    detours = first | ((odd == 1) & (me_x < nx - 1))
    carries = (me_x == 1) | ((odd == 0) & (me_x < nx - 2))

    barrier = pltpu.get_barrier_semaphore()

    def greet(device, sem=barrier):
        pl.semaphore_signal(sem, inc=1, device_id=device, device_id_type=MESH)

    for device in (near, on_y(1), on_y(ny - 1)):
        greet(device)

    @pl.when((odd == 1) & jnp.logical_not(last))
    def _():
        greet(far)

    @pl.when((odd == 0) & (me_x > 0))
    def _():
        greet(on_x(nx - 2))

    load_section = pltpu.make_async_copy(section, sec, load_sem.at[0])
    load_start = pltpu.make_async_copy(start, old, load_sem.at[1])
    load_start.start()
    load_section.start()

    direct = old.shape[0] - DETOUR

    def remote(src, dst, send_sem, recv_sem, device):
        return pltpu.make_async_remote_copy(
            src_ref=src,
            dst_ref=dst,
            send_sem=send_sem,
            recv_sem=recv_sem,
            device_id=device,
            device_id_type=MESH,
        )

    slabs = [(t, 0, WIDTH) for t in range(tiles - 1)]
    slabs += [(tiles - 1, 1, WIDTH - 1), (tiles - 1, 0, 1)]

    def layers_of(side, h, count):
        return pl.ds(h + side * (WIDTH - 2 * h - count), count)

    def edge_of(side, t, comps, h=0, count=WIDTH):
        layers = layers_of(side, h, count)
        layers = pl.ds((1 - side) * (cx - WIDTH) + layers.start, count)
        return old.at[comps, layers, pl.ds(t * ROWS, ROWS), :]

    def near_copy(n, side):
        t, h, count = slabs[n]
        every = pl.ds(0, old.shape[0] - (n == 0))
        return remote(
            edge_of(odd, t, every, h, count),
            xhalo.at[side, t, every, layers_of(side, h, count)],
            ns_sem.at[n], nr_sem.at[n], near,
        )

    def near_rest_copy(side):
        rest = pl.ds(old.shape[0] - 1, 1)
        return remote(
            edge_of(odd, 0, rest), xhalo.at[side, 0, rest], sides_sem.at[0], sider_sem.at[0], near
        )

    def sidestep_copy():
        rest = pl.ds(old.shape[0] - 1, 1)
        return remote(edge_of(odd, 0, rest), aside, sides_sem.at[0], sider_sem.at[1], far)

    def step_copy():
        rest = pl.ds(old.shape[0] - 1, 1)
        return remote(aside, xhalo.at[0, 0, rest], sides_sem.at[1], sider_sem.at[0], on_x(2))

    def far_copy(n, side):
        t, h, count = slabs[n]
        some = pl.ds(0, direct)
        return remote(
            edge_of(1 - odd, t, some, h, count),
            xhalo.at[side, t, some, layers_of(side, h, count)],
            fs_sem.at[n], fr_sem.at[n], far,
        )

    def rest_copy(t, side):
        rest = pl.ds(direct, DETOUR)
        return remote(
            edge_of(1 - odd, t, rest), xhalo.at[side, t, rest], ds_sem.at[t], dr_sem.at[t], far
        )

    def detour_copy(t):
        rest = pl.ds(direct, DETOUR)
        return remote(edge_of(1 - odd, t, rest), relay.at[t], ds_sem.at[t], rr_sem.at[t], near)

    def carry_copy(t):
        rest = pl.ds(direct, DETOUR)
        return remote(
            relay.at[t], xhalo.at[odd, t, rest], rs_sem.at[t], dr_sem.at[t], beyond
        )

    def y_copy(side):
        rows = pl.ds(cy - ROWS, ROWS) if side == 0 else pl.ds(0, ROWS)
        return pltpu.make_async_remote_copy(
            src_ref=old.at[:, :, rows, :],
            dst_ref=ylo if side == 0 else yhi,
            send_sem=ys_sem.at[side],
            recv_sem=yr_sem.at[side],
            device_id=on_y(1) if side == 0 else on_y(ny - 1),
            device_id_type=MESH,
        )

    def start_far():
        for n in range(len(slabs)):
            far_copy(n, 1 - odd).start()

        @pl.when(jnp.logical_not(detours))
        def _():
            for t in range(tiles):
                rest_copy(t, 1 - odd).start()

    told = jnp.where(first | ((odd == 1) & jnp.logical_not(last)), 3, 4)
    pl.semaphore_wait(barrier, told + jnp.where((odd == 0) & (me_x < nx - 2), 1, 0))

    @pl.when(first)
    def _():
        greet(far)

    @pl.when(((odd == 0) & (me_x > 0)) | last)
    def _():
        greet(far, ring_sem.at[0])

    @pl.when(last)
    def _():
        greet(on_x(2), ring_sem.at[1])

    load_start.wait()

    @pl.when(detours)
    def _():
        for t in range(tiles):
            detour_copy(t).start()

    @pl.when(sidesteps)
    def _():
        sidestep_copy().start()

    @pl.when(jnp.logical_not(sidesteps))
    def _():
        near_rest_copy(odd).start()

    for n in range(len(slabs)):
        near_copy(n, odd).start()

    @pl.when(((odd == 0) & (me_x > 0)) | last)
    def _():
        start_far()

    for side in range(2):
        y_copy(side).start()

    @pl.when((odd == 1) & jnp.logical_not(last))
    def _():
        pl.semaphore_wait(ring_sem.at[0], 1)
        start_far()

    rounds = meeting_rounds(nx, ny)

    def meet(r):
        axis, distance = rounds[r]
        for k in (distance, -distance):
            device = on_x(nx + k) if axis == "gx" else on_y(ny + k)
            pl.semaphore_signal(meet_sem.at[r], inc=1, device_id=device, device_id_type=MESH)

    def met(r):
        pl.semaphore_wait(meet_sem.at[r], 2)
        if r + 1 < len(rounds):
            meet(r + 1)

    scale = 0.25 * (COURANT / speed[0, 0])

    edge = jnp.zeros((WIDTH, cy, nz), jnp.float32)
    for c in range(5):
        fx[c, 0:WIDTH] = edge
        fx[c, cx + WIDTH : cx + 2 * WIDTH] = edge
    for c in range(4):
        sm[c, 0:WIDTH, ROWS : ROWS + cy] = edge
        sm[c, cx + WIDTH : cx + 2 * WIDTH, ROWS : ROWS + cy] = edge

    load_section.wait()

    def along_z(i, _):
        q = [sec[c, i] for c in range(5)]
        prim = primitive(q)
        smooth = smooth_terms(prim)
        for c, term in enumerate(flux_terms(q, prim, 0)):
            fx[c, i + WIDTH] = term
        for c, term in enumerate(flux_terms(q, prim, 1)):
            fy[c, i, ROWS : ROWS + cy] = term
        for c, term in enumerate(smooth):
            sm[c, i + WIDTH, ROWS : ROWS + cy] = term
        for c, term in enumerate(flux_terms(q, prim, 2)):
            total = None
            for m in range(1, WIDTH + 1):
                f = FIRST[m - 1] * term
                if c > 0:
                    s = SECOND[m - 1] * smooth[c - 1]
                    above, below = s - f, s + f
                else:
                    above, below = -f, f
                pair = pltpu.roll(above, nz - m, 1) + pltpu.roll(below, m, 1)
                total = pair if total is None else total + pair
            if c > 0:
                total = total + (3.0 * CENTRE) * smooth[c - 1]
            acc[c, i] = total
        return 0

    lax.fori_loop(0, cx, along_z, 0)

    @pl.when(me_x == 1)
    def _():
        pl.semaphore_wait(ring_sem.at[1], 1)

    @pl.when(first)
    def _():
        pl.semaphore_wait(ring_sem.at[0], 1)
        start_far()

    @pl.when(steps)
    def _():
        sidestep_copy().wait_recv()
        step_copy().start()

    @pl.when(carries)
    def _():
        for t in range(tiles):
            detour_copy(t).wait_recv()
            carry_copy(t).start()

    meet(0)

    def along_x(i, _):
        for c in range(5):
            total = acc[c, i]
            for m in range(1, WIDTH + 1):
                total = total - FIRST[m - 1] * (fx[c, i + WIDTH + m] - fx[c, i + WIDTH - m])
                if c > 0:
                    total = total + SECOND[m - 1] * (
                        sm[c - 1, i + WIDTH + m, ROWS : ROWS + cy]
                        + sm[c - 1, i + WIDTH - m, ROWS : ROWS + cy]
                    )
            acc[c, i] = total
        return 0

    lax.fori_loop(0, cx, along_x, 0)
    met(0)
    met(1)

    y_copy(0).wait_recv()
    y_copy(1).wait_recv()

    def along_y(i, _):
        for halo, first in ((ylo, 0), (yhi, ROWS + cy)):
            q = [halo[c, i] for c in range(5)]
            prim = primitive(q)
            for c, term in enumerate(flux_terms(q, prim, 1)):
                fy[c, i, first : first + ROWS] = term
            for c, term in enumerate(smooth_terms(prim)):
                sm[c, i + WIDTH, first : first + ROWS] = term
        for c in range(5):
            total = acc[c, i]
            for m in range(1, WIDTH + 1):
                above, below = ROWS + m, ROWS - m
                total = total - FIRST[m - 1] * (
                    fy[c, i, above : above + cy] - fy[c, i, below : below + cy]
                )
                if c > 0:
                    total = total + SECOND[m - 1] * (
                        sm[c - 1, i + WIDTH, above : above + cy]
                        + sm[c - 1, i + WIDTH, below : below + cy]
                    )
            acc[c, i] = total
        return 0

    lax.fori_loop(0, cx, along_y, 0)
    met(2)
    for r in range(3, len(rounds)):
        met(r)

    largest = None
    for n, (t, first_h, count) in enumerate(slabs):
        ends = n + 1 == len(slabs) or slabs[n + 1][0] != t
        rows = slice(t * ROWS, (t + 1) * ROWS)
        if count == 1:
            far_copy(n, odd).wait_recv()
            near_copy(n, 1 - odd).wait_recv()
        for turn in range(2):
            if turn == 0:
                side = odd
                if count > 1:
                    far_copy(n, side).wait_recv()
                if first_h + count == WIDTH:
                    rest_copy(t, side).wait_recv()
            else:
                side = 1 - odd
                if count > 1:
                    near_copy(n, side).wait_recv()
                if n == 0:
                    near_rest_copy(side).wait_recv()
            sign = (1 - 2 * side).astype(jnp.float32)
            inner = [side * (cx - 1 - 2 * i) + i for i in range(WIDTH)]
            touched = range(first_h + count)
            totals = [[acc[c, inner[i], rows] for c in range(5)] for i in touched]
            for h in range(first_h, first_h + count):
                q = [xhalo[side, t, c, side * (WIDTH - 1 - 2 * h) + h] for c in range(5)]
                prim = primitive(q)
                flux = [sign * f for f in flux_terms(q, prim, 0)]
                smooth = smooth_terms(prim)
                for i in range(h + 1):
                    m = i + WIDTH - h
                    for c in range(5):
                        term = FIRST[m - 1] * flux[c]
                        if c > 0:
                            term = term + SECOND[m - 1] * smooth[c - 1]
                        totals[i][c] = totals[i][c] + term
            for i in touched:
                if not ends and i < first_h:
                    for c in range(5):
                        acc[c, inner[i], rows] = totals[i][c]
                    continue
                new = []
                for c in range(5):
                    value = (
                        0.75 * old[c, inner[i], rows]
                        + 0.25 * sec[c, inner[i], rows]
                        + scale * totals[i][c]
                    )
                    out[c, inner[i], rows] = value
                    new.append(value)
                wave = wave_speed(new)
                largest = wave if largest is None else jnp.maximum(largest, wave)

    me = me_x * ny + me_y

    def top_copy(k):
        to = k + (k >= me).astype(jnp.int32)
        return remote(top, got.at[me], ts_sem, tr_sem, (to // ny, lax.rem(to, ny)))

    def every_top():
        others = pl.ds(0, devices - 1)
        return remote(got.at[others], got.at[others], ts_sem, tr_sem, near)

    folded = largest[:, 0:128]
    for first in range(128, nz, 128):
        folded = jnp.maximum(folded, largest[:, first : first + 128])
    peak = jnp.max(folded, axis=0, keepdims=True)
    top[...] = peak

    def send(k, _):
        top_copy(k).start()
        return 0

    lax.fori_loop(0, devices - 1, send, 0, unroll=devices <= 64)
    got[me] = peak
    for n in range(len(slabs)):
        near_copy(n, odd).wait_send()
        far_copy(n, 1 - odd).wait_send()
    for t in range(tiles):
        rest_copy(t, 1 - odd).wait_send()

    near_rest_copy(odd).wait_send()

    @pl.when(steps)
    def _():
        step_copy().wait_send()

    @pl.when(carries)
    def _():
        for t in range(tiles):
            carry_copy(t).wait_send()

    for side in range(2):
        y_copy(side).wait_send()

    every_top().wait_send()
    every_top().wait_recv()
    peak = jnp.max(got[...], axis=0)
    next_speed[...] = jnp.broadcast_to(jnp.max(peak, axis=1, keepdims=True), next_speed.shape)


def finish(state, peak, new_state, next_speed, sem):
    comps = state.shape[0]
    copies = [
        pltpu.make_async_copy(state.at[c], new_state.at[c], sem.at[c]) for c in range(comps)
    ]
    copies.append(pltpu.make_async_copy(peak, next_speed, sem.at[comps]))
    for copy in copies:
        copy.start()
    for copy in copies:
        copy.wait()


def local(nx, ny, start_state, section_state, previous_speed):
    comps, cx, cy, nz = section_state.shape
    tiles = cy // ROWS
    f32 = jnp.float32
    dma = pltpu.SemaphoreType.DMA
    state, peak = pl.pallas_call(
        functools.partial(kernel, nx, ny),
        out_shape=(
            pltpu.VMEM(section_state.shape, f32),
            pltpu.VMEM((1, 128), f32),
        ),
        in_specs=[
            pl.BlockSpec(memory_space=pl.ANY),
            pl.BlockSpec(memory_space=pl.ANY),
            pl.BlockSpec(memory_space=pltpu.SMEM),
        ],
        out_specs=(
            pl.BlockSpec(memory_space=pltpu.VMEM),
            pl.BlockSpec(memory_space=pltpu.VMEM),
        ),
        scratch_shapes=[
            pltpu.VMEM(section_state.shape, f32),
            pltpu.VMEM(section_state.shape, f32),
            pltpu.VMEM(section_state.shape, f32),
            pltpu.VMEM((comps, cx + 2 * WIDTH, cy, nz), f32),
            pltpu.VMEM((comps, cx, cy + 2 * ROWS, nz), f32),
            pltpu.VMEM((comps - 1, cx + 2 * WIDTH, cy + 2 * ROWS, nz), f32),
            pltpu.VMEM((2, tiles, comps, WIDTH, ROWS, nz), f32),
            pltpu.VMEM((tiles, DETOUR, WIDTH, ROWS, nz), f32),
            pltpu.VMEM((1, WIDTH, ROWS, nz), f32),
            pltpu.VMEM((comps, cx, ROWS, nz), f32),
            pltpu.VMEM((comps, cx, ROWS, nz), f32),
            pltpu.VMEM((1, 128), f32),
            pltpu.VMEM((nx * ny, 1, 128), f32),
            dma((2,)),
            dma((tiles + 1,)),
            dma((tiles + 1,)),
            dma((tiles + 1,)),
            dma((tiles + 1,)),
            dma((tiles,)),
            dma((tiles,)),
            dma((tiles,)),
            dma((tiles,)),
            dma((2,)),
            dma((2,)),
            dma((2,)),
            dma((2,)),
            dma,
            dma,
            pltpu.SemaphoreType.REGULAR((len(meeting_rounds(nx, ny)),)),
            pltpu.SemaphoreType.REGULAR((2,)),
        ],
        compiler_params=pltpu.CompilerParams(collective_id=0, has_side_effects=True),
        name="section_step",
    )(start_state, section_state, previous_speed.reshape(1, 1))
    new_state, next_speed = pl.pallas_call(
        finish,
        out_shape=(
            jax.ShapeDtypeStruct(section_state.shape, f32),
            jax.ShapeDtypeStruct((1, 128), f32),
        ),
        in_specs=[pl.BlockSpec(memory_space=pltpu.VMEM)] * 2,
        out_specs=(pl.BlockSpec(memory_space=pl.ANY), pl.BlockSpec(memory_space=pl.ANY)),
        scratch_shapes=[dma((comps + 1,))],
        name="write_out",
    )(
        pltpu.with_memory_space_constraint(state, pltpu.VMEM),
        pltpu.with_memory_space_constraint(peak, pltpu.VMEM),
    )
    return new_state, next_speed[0, 0]


def solution(mesh):
    nx, ny = mesh.shape["gx"], mesh.shape["gy"]
    in_specs = (P(None, "gx", "gy", None), P(None, "gx", "gy", None), P())
    out_specs = (P(None, "gx", "gy", None), P())
    return jax.shard_map(
        functools.partial(local, nx, ny),
        mesh=mesh,
        in_specs=in_specs,
        out_specs=out_specs,
        check_vma=False,
    )
```
